32 devices in a mesh: grp: 4 (over x, core), row: 4 (over z), col: 2 (over y).
Axes of the slice: x: 2, y: 2, z: 4, core: 2. Of those that a mesh axis runs over, the one named last changes fastest.
Arguments:
- fields: bfloat16 [4, 4, 192, 1536], P('grp', None, 'row', 'col'), may hold values from -12 to 12
- offset: int32 [1], replicated, may hold values from 0 to 191
- level_index: int32 [4], replicated, may hold values from 0 to 3, each once
- nudge_rate: float32 [4], replicated, may hold values from 0.2 to 0.9
- driving: float32 [4, 64, 64], replicated, may hold values from -4 to 4
Outputs:
- nudged: bfloat16 [4, 4, 192, 1536], P('grp', None, 'row', 'col')
The draws below stay inside these ranges and needn't reach their ends.
Inputs may be any that keep to these rules, and one draw needn't show every extreme that they name: `offset`: the footprint covers a third of the parent rows from there on, wrapping around the periodic domain. `level_index`: each parent level is fed by exactly one child level.
All inputs are finite; a program needn't handle non-finite values.
Results may differ from the reference program's by a relative error of at most 0.0034.
Values may be sent and summed in bfloat16 or wider, within the bound.
No kernel may reach another device: no remote copies, remote signals or barrier semaphores. Data moves between devices by JAX's collectives and lax.ppermute only.
A program may use at most 64 MiB of HBM per device.

```python
import math
import jax
import jax.numpy as jnp
from jax import lax

LEVELS = 4
TILE_COLS = 768
MAX_WAVE = 32
BASIS = 64
PARENT_ROWS = 192
PARENT_COLS = 1536
N_GRP = 4


def fourier_table_drawn(positions, cell_count, max_order):
    orders = jnp.arange(1, max_order + 1, dtype=jnp.int32)
    period = 3 * cell_count
    phase_index = positions[:, None] * orders[None, :] % period
    angles = phase_index.astype(jnp.float32) * jnp.float32(2.0 * math.pi / period)
    wave_scale = jnp.float32(math.sqrt(2.0 / cell_count))
    constant = jnp.full((positions.shape[0], 1), 1.0 / math.sqrt(cell_count), jnp.float32)
    return jnp.concatenate([constant, wave_scale * jnp.cos(angles), wave_scale * jnp.sin(angles[:, :max_order - 1])], axis=1)


def draw_fields(key, part):
    key_noise = jax.random.fold_in(key, 11)
    key_parent = jax.random.fold_in(key, 12)
    key_child = jax.random.fold_in(key, 13)
    amplitude = math.sqrt(PARENT_ROWS * PARENT_COLS) / BASIS
    row_ids = jnp.arange(PARENT_ROWS, dtype=jnp.int32)
    col_ids = jnp.arange(PARENT_COLS, dtype=jnp.int32)
    row_table = fourier_table_drawn(3 * row_ids, PARENT_ROWS, MAX_WAVE)
    col_table = fourier_table_drawn(3 * col_ids, PARENT_COLS, MAX_WAVE)
    child_row_table = fourier_table_drawn((row_ids - 1) % (3 * PARENT_ROWS), PARENT_ROWS, MAX_WAVE)
    tile_ids = col_ids // TILE_COLS
    within = col_ids % TILE_COLS
    child_col_tables = jnp.stack([fourier_table_drawn(((3 * tile_ids + slot) * TILE_COLS + within - 1) % (3 * PARENT_COLS), PARENT_COLS, MAX_WAVE) for slot in range(3)])
    shape = (N_GRP, LEVELS, PARENT_ROWS, PARENT_COLS)
    noise_part = jax.random.normal(key_noise, shape, jnp.float32)
    parent_coef = jax.random.normal(key_parent, (LEVELS, BASIS, BASIS), jnp.float32) * amplitude
    child_coef = jax.random.normal(key_child, (LEVELS, BASIS, BASIS), jnp.float32) * amplitude
    parent_cols = jnp.einsum('lnm,jm->lnj', parent_coef, col_table)
    parent_smooth = jnp.einsum('in,lnj->lij', row_table, parent_cols)
    child_cols = jnp.einsum('lnm,gjm->glnj', child_coef, child_col_tables)
    child_smooth = jnp.einsum('in,glnj->glij', child_row_table, child_cols)
    smooth_part = jnp.concatenate([child_smooth, parent_smooth[None]], axis=0)
    total = jnp.clip(smooth_part + noise_part, -12.0, 12.0)
    return total.astype(jnp.bfloat16)


def noise(own_key, shape, scale, most, held_as=jnp.bfloat16):
    return jnp.clip(scale * jax.random.normal(own_key, shape, jnp.float32), -most, most).astype(held_as)


def setup_inputs(seed: int = 0) -> dict:
    key_of = jax.random.split(jax.random.key(seed), 6)
    fields = draw_fields(jax.random.fold_in(key_of[5], 71), 0)
    offset = jax.random.randint(key_of[1], (1,), 0, PARENT_ROWS).astype(jnp.int32)
    level_index = jax.random.permutation(key_of[2], LEVELS).astype(jnp.int32)
    nudge_rate = jnp.clip(jnp.exp(jax.random.uniform(key_of[3], (LEVELS,), jnp.float32, math.log(0.2), math.log(0.9))), 0.2, 0.9)
    driving = noise(key_of[4], (LEVELS, BASIS, BASIS), 1.0, 4.0, jnp.float32)
    return {"fields": fields, "offset": offset, "level_index": level_index, "nudge_rate": nudge_rate, "driving": driving}


def fourier_table(positions, cell_count, max_order):
    orders = jnp.arange(1, max_order + 1, dtype=jnp.int32)
    period = 3 * cell_count
    phase_index = positions[:, None] * orders[None, :] % period
    angles = phase_index.astype(jnp.float32) * jnp.float32(2.0 * math.pi / period)
    wave_scale = jnp.float32(math.sqrt(2.0 / cell_count))
    constant = jnp.full((positions.shape[0], 1), 1.0 / math.sqrt(cell_count), jnp.float32)
    return jnp.concatenate([constant, wave_scale * jnp.cos(angles), wave_scale * jnp.sin(angles[:, :max_order - 1])], axis=1)

def reference(fields, offset, level_index, nudge_rate, driving):
    shift_rows = offset[0]
    level_ids = jnp.arange(LEVELS, dtype=jnp.int32)
    inverse = lax.optimization_barrier(jnp.sum(level_ids[:, None] * (level_index[:, None] == level_ids[None, :]).astype(jnp.int32), axis=0))
    row_ids = jnp.arange(PARENT_ROWS, dtype=jnp.int32)
    col_ids = jnp.arange(PARENT_COLS, dtype=jnp.int32)
    row_table = fourier_table(3 * row_ids, PARENT_ROWS, MAX_WAVE)
    col_table = fourier_table(3 * col_ids, PARENT_COLS, MAX_WAVE)
    row_half = lax.optimization_barrier(row_table.astype(jnp.bfloat16))
    row_rounded = row_half.astype(jnp.float32)
    col_rounded = col_table.astype(jnp.bfloat16)
    child_row_table = fourier_table((3 * shift_rows + row_ids - 1) % (3 * PARENT_ROWS), PARENT_ROWS, MAX_WAVE)
    tile_ids = col_ids // TILE_COLS
    within = col_ids % TILE_COLS
    child_col_tables = jnp.stack([fourier_table(((3 * tile_ids + slot) * TILE_COLS + within - 1) % (3 * PARENT_COLS), PARENT_COLS, MAX_WAVE) for slot in range(3)])
    amplitude = math.sqrt(PARENT_ROWS * PARENT_COLS) / BASIS
    strip_index = (row_ids - shift_rows) % PARENT_ROWS
    covered = strip_index < PARENT_ROWS // 3
    strip_rows = jnp.clip(strip_index, 0, PARENT_ROWS // 3 - 1)

    def one_level(parent_level):
        child_level = inverse[parent_level]
        child_slots = lax.dynamic_index_in_dim(fields[:N_GRP - 1], child_level, axis=1, keepdims=False)
        parent = lax.dynamic_index_in_dim(fields[N_GRP - 1], parent_level, axis=0, keepdims=False)
        block_sums = lax.optimization_barrier(jnp.sum(child_slots.reshape(3, PARENT_ROWS // 3, 3, PARENT_COLS // 3, 3), axis=(2, 4), dtype=jnp.float32))
        averaged = (block_sums / 9.0).astype(jnp.bfloat16)
        averaged = averaged.reshape(3, PARENT_ROWS // 3, PARENT_COLS // TILE_COLS, TILE_COLS // 3)
        averaged = jnp.transpose(averaged, (1, 2, 0, 3)).reshape(PARENT_ROWS // 3, PARENT_COLS)
        fed_tile = jnp.where(covered[:, None], averaged[strip_rows], parent)
        projected = jnp.dot(fed_tile, col_rounded, preferred_element_type=jnp.float32)
        coeffs = jnp.dot(row_rounded.T, projected, precision=lax.Precision.HIGHEST)
        deficit = amplitude * driving[parent_level] - coeffs
        rate = nudge_rate[parent_level]
        spread_cols = jnp.dot(deficit, col_table.T, precision=lax.Precision.HIGHEST)
        increment = jnp.dot(row_table, spread_cols, precision=lax.Precision.HIGHEST)
        parent_new = (fed_tile.astype(jnp.float32) + rate * increment).astype(jnp.bfloat16)
        child_spread = jnp.einsum('nm,gjm->gnj', deficit, child_col_tables, precision=lax.Precision.HIGHEST)
        child_increment = jnp.einsum('in,gnj->gij', child_row_table, child_spread, precision=lax.Precision.HIGHEST)
        child_new = (child_slots.astype(jnp.float32) + rate * child_increment).astype(jnp.bfloat16)
        return (parent_new, child_new)
    parents, children = lax.map(one_level, level_ids)
    children = jnp.take(children, level_index, axis=0)
    children = jnp.transpose(children, (1, 0, 2, 3))
    return jnp.concatenate([children, parents[None]], axis=0)
```

```python
import functools
import math

import jax
import jax.numpy as jnp
import numpy as np
from jax import lax
from jax.experimental import pallas as pl
from jax.experimental.pallas import tpu as pltpu
from jax.sharding import PartitionSpec as P

MAX_WAVE = 32
BASIS = 2 * MAX_WAVE
AXES = ("grp", "row", "col")
VMEM = pl.BlockSpec(memory_space=pltpu.VMEM)
SMEM = pl.BlockSpec(memory_space=pltpu.SMEM)
ANY = pl.BlockSpec(memory_space=pl.ANY)


def basis_table(positions, cell_count):
    period = 3 * cell_count
    orders = np.arange(1, MAX_WAVE + 1)
    angles = (np.asarray(positions)[:, None] * orders % period) * (2.0 * math.pi / period)
    scale = math.sqrt(2.0 / cell_count)
    constant = np.full((len(positions), 1), 1.0 / math.sqrt(cell_count))
    table = np.concatenate([constant, scale * np.cos(angles), scale * np.sin(angles[:, :-1])], 1)
    return table.astype(np.float32)


def halves(table):
    high = table.astype(jnp.bfloat16)
    return high, (table - high.astype(np.float32)).astype(jnp.bfloat16)


def split(value):
    high = value.astype(jnp.bfloat16)
    return high, (value - high.astype(jnp.float32)).astype(jnp.bfloat16)


def dot(a, b, contract=((1,), (0,))):
    return lax.dot_general(a, b, (contract, ((), ())), preferred_element_type=jnp.float32)


def parity_of_device():
    bits = lax.axis_index("grp") ^ lax.axis_index("row") ^ lax.axis_index("col")
    for shift in (8, 4, 2, 1):
        bits = bits ^ (bits >> shift)
    return bits & 1


def inverse_of(level_ref, parent_level, levels):
    found = jnp.int32(0)
    for level in range(levels):
        found = found + jnp.where(level_ref[level] == parent_level, level, 0)
    return found


def first_kernel(
    full_rows, groups, offset, level_index, tile_hbm, cols_hbm, rows_hbm,
    averaged, keep, send, tile, cols, rows, sums, coeffs, sems,
):
    levels, tile_rows, tile_cols = tile.shape
    third_rows, third_cols = tile_rows // 3, tile_cols // 3
    group, row, col = (lax.axis_index(a) for a in AXES)
    copies = [
        pltpu.make_async_copy(tile_hbm, tile, sems.at[0]),
        pltpu.make_async_copy(cols_hbm.at[col], cols, sems.at[1]),
        pltpu.make_async_copy(rows_hbm, rows, sems.at[2]),
    ]
    for copy in copies:
        copy.start()
    shift = offset[0]
    for copy in copies:
        copy.wait()

    def project(blocks, table, weights):
        left = lax.broadcasted_iota(jnp.int32, table.shape, 1) < BASIS
        zero = jnp.zeros_like(table)
        first, second = jnp.where(left, table, zero), jnp.where(left, zero, table)
        for pair in range(levels // 2):
            projected = dot(blocks[2 * pair], first) + dot(blocks[2 * pair + 1], second)
            high, low = split(projected)
            rows_first = ((0,), (0,))
            coeffs[pair] = dot(weights, high, rows_first) + dot(weights, low, rows_first)

    @pl.when(group < groups - 1)
    def _():
        lanes = sums.shape[-1]
        depth = 3 * lanes
        cell = lax.broadcasted_iota(jnp.int32, (depth, lanes), 0)
        block = 3 * lax.broadcasted_iota(jnp.int32, (depth, lanes), 1)
        pick = jnp.where((cell >= block) & (cell < block + 3), 1.0, 0.0).astype(jnp.bfloat16)
        flat = tile[...].reshape(levels * tile_rows, tile_cols)
        for part in range(third_cols // lanes):
            piece = dot(flat[:, part * depth : (part + 1) * depth], pick)
            sums[part] = piece.reshape(levels, tile_rows, lanes)
        blocks = []
        for parent_level in range(levels):
            level = inverse_of(level_index, parent_level, levels)
            totals = [
                sum(sums[part, level, pl.ds(a, third_rows, 3), :] for a in range(3))
                for part in range(third_cols // lanes)
            ]
            block = (jnp.concatenate(totals, axis=1) * (1.0 / 9.0)).astype(jnp.bfloat16)
            averaged[:, parent_level * third_cols : (parent_level + 1) * third_cols] = block
            blocks.append(block)
        table = cols[pl.ds(pl.multiple_of(group * third_cols, third_cols), third_cols), :]
        start = lax.rem(row * third_rows + shift, full_rows)
        project(blocks, table, rows[pl.ds(start, third_rows), :].astype(jnp.bfloat16))

    @pl.when(group == groups - 1)
    def _():
        averaged[...] = jnp.zeros_like(averaged)
        cell = lax.broadcasted_iota(jnp.int32, (tile_rows, BASIS), 0)
        strip = lax.rem(row * tile_rows + cell - shift + full_rows, full_rows)
        weights = rows[pl.ds(pl.multiple_of(row * tile_rows, 8), tile_rows), :]
        weights = jnp.where(strip < full_rows // 3, 0.0, weights).astype(jnp.bfloat16)
        project([tile[level] for level in range(levels)], cols[...], weights)

    half = parity_of_device()
    keep[...] = coeffs[half]
    send[...] = coeffs[1 - half]


def select_kernel(full_rows, offset, *refs):
    *blocks, out = refs
    tile_rows, third_rows = out.shape[0], blocks[0].shape[0]
    row = lax.axis_index("row")
    shape = (tile_rows, third_rows * len(blocks))
    cell = lax.broadcasted_iota(jnp.int32, shape, 0)
    wanted = lax.rem(row * tile_rows + cell - offset[0] + full_rows, full_rows)
    place = lax.broadcasted_iota(jnp.int32, shape, 1)
    held = (row ^ (place // third_rows)) * third_rows + place % third_rows
    pick = jnp.where(wanted == held, 1.0, 0.0).astype(jnp.bfloat16)
    strip = jnp.concatenate([block[...] for block in blocks], axis=0)
    out[...] = dot(pick, strip).astype(jnp.bfloat16)


def prepare_kernel(
    full_rows, amplitude, groups, columns, after, offset, tile_hbm, spread_hbm, child_rows_hbm,
    parent_rows_hbm, driving_hbm, tile, spread, weights, target, rows, driving, sems,
):
    levels, tile_rows, _ = tile.shape
    group, row, col = (lax.axis_index(a) for a in AXES)
    is_parent = group == groups - 1
    slot = jnp.where(is_parent, (groups - 1) * columns + col, col * (groups - 1) + group)
    quarters = [
        pltpu.make_async_copy(
            spread_hbm.at[slot, part // 2], spread.at[pl.ds(part * BASIS, BASIS)], sems.at[part]
        )
        for part in range(4)
    ]
    copies = quarters + [
        pltpu.make_async_copy(tile_hbm, tile, sems.at[4]),
        pltpu.make_async_copy(driving_hbm, driving, sems.at[5]),
        pltpu.make_async_copy(child_rows_hbm, rows.at[pl.ds(0, child_rows_hbm.shape[0])], sems.at[6]),
        pltpu.make_async_copy(
            parent_rows_hbm,
            rows.at[pl.ds(child_rows_hbm.shape[0], parent_rows_hbm.shape[0])],
            sems.at[7],
        ),
    ]
    for copy in copies:
        copy.start()
    for copy in copies:
        copy.wait()
    period = 3 * full_rows
    child_start = lax.rem(3 * offset[0] + row * tile_rows - 1 + period, period)
    parent_start = child_rows_hbm.shape[0] + row * tile_rows
    weights[...] = rows[pl.ds(jnp.where(is_parent, parent_start, child_start), tile_rows), :]
    for pair in range(levels // 2):
        target[pair] = amplitude * jnp.concatenate(
            [driving[2 * pair], driving[2 * pair + 1]], axis=1
        )


def final_kernel(
    full_rows, groups, offset, level_index, rate, mine, other, tile, spread, weights, target,
    block_0, block_1, block_2, out_hbm, deficit, left, base, result, sems,
):
    levels, tile_rows, tile_cols = base.shape
    third_cols = tile_cols // 3
    group, row = lax.axis_index("grp"), lax.axis_index("row")
    is_parent = group == groups - 1
    half = parity_of_device()
    deficit[half] = target[half] - mine[...]
    deficit[1 - half] = target[1 - half] - other[...]
    is_left = lax.broadcasted_iota(jnp.int32, (tile_rows, 2 * BASIS), 1) < BASIS
    for pair in range(levels // 2):
        turned = jnp.dot(
            weights[...], deficit[pair], precision=lax.Precision.HIGHEST,
            preferred_element_type=jnp.float32,
        )
        for side in range(2):
            parent_level = 2 * pair + side
            high, low = split(turned * rate[parent_level])
            low = pltpu.roll(low.astype(jnp.float32), BASIS, 1).astype(jnp.bfloat16)
            here = is_left if side == 0 else ~is_left
            span = pl.ds(parent_level * tile_rows, tile_rows)
            left[span, : 2 * BASIS] = jnp.where(here, high, low)
            left[span, 2 * BASIS :] = jnp.where(here, high, jnp.zeros_like(high))
    increment = dot(left[...], spread[...])

    @pl.when(is_parent)
    def _():
        cell = lax.broadcasted_iota(jnp.int32, (tile_rows, third_cols), 0)
        strip = lax.rem(row * tile_rows + cell - offset[0] + full_rows, full_rows)
        covered = strip < full_rows // 3
        for level in range(levels):
            for third, block in enumerate((block_0, block_1, block_2)):
                span = slice(third * third_cols, (third + 1) * third_cols)
                arrived = block[:, level * third_cols : (level + 1) * third_cols]
                base[level, :, span] = jnp.where(
                    covered, arrived.astype(jnp.float32), tile[level, :, span].astype(jnp.float32)
                )

    @pl.when(jnp.logical_not(is_parent))
    def _():
        base[...] = tile[...].astype(jnp.float32)

    copies = []
    for parent_level in range(levels):
        level = jnp.where(is_parent, parent_level, inverse_of(level_index, parent_level, levels))
        rows = increment[parent_level * tile_rows : (parent_level + 1) * tile_rows]
        result[level] = (base[level] + rows).astype(jnp.bfloat16)
        copy = pltpu.make_async_copy(
            result.at[level], out_hbm.at[level], sems.at[parent_level]
        )
        copy.start()
        copies.append(copy)
    for copy in copies:
        copy.wait()


def per_device(sizes, fields, offset, level_index, nudge_rate, driving):
    groups, row_count, col_count = sizes
    tile_in = fields[0]
    levels, tile_rows, tile_cols = tile_in.shape
    third_rows, third_cols = tile_rows // 3, tile_cols // 3
    full_rows, full_cols = row_count * tile_rows, col_count * tile_cols
    f32, bf16 = jnp.float32, jnp.bfloat16

    cols = basis_table(3 * np.arange(full_cols), full_cols)
    cols_twice = np.concatenate([cols, cols], 1).reshape(col_count, tile_cols, 2 * BASIS)
    cols_twice = cols_twice.astype(bf16)
    parent_rows = basis_table(3 * np.arange(full_rows), full_rows)
    rounded = parent_rows.astype(bf16).astype(np.float32)
    rounded = np.concatenate([rounded, rounded[:third_rows]], 0)
    child_rows = basis_table(np.arange(3 * full_rows), full_rows)
    child_rows = np.concatenate([child_rows, child_rows[:tile_rows]], 0)
    child_cols = basis_table((np.arange(3 * full_cols) - 1) % (3 * full_cols), full_cols)
    spread_rows = np.concatenate([child_cols, cols], 0).reshape(-1, tile_cols, BASIS)
    spread_rows = spread_rows.transpose(0, 2, 1)
    spread_table = np.stack(halves(spread_rows), 1)
    amplitude = math.sqrt(full_rows * full_cols) / BASIS

    def mask_of(group_bits, row_bits, col_bits):
        return (group_bits * row_count + row_bits) * col_count + col_bits

    def exchange(value, mask):
        count = groups * row_count * col_count
        return lax.ppermute(value, AXES, [(i, i ^ mask) for i in range(count)])

    flip = mask_of(1, 0, 0)
    rounds = [mask_of(1 << k, 0, 0) ^ flip for k in range(1, groups.bit_length() - 1)]
    rounds += [mask_of(0, 0, 1 << k) ^ flip for k in range(col_count.bit_length() - 1)]
    rounds += [mask_of(0, 1 << k, 0) ^ flip for k in range(row_count.bit_length() - 1)]

    averaged, keep, send = pl.pallas_call(
        functools.partial(first_kernel, full_rows, groups),
        out_shape=(
            jax.ShapeDtypeStruct((third_rows, levels * third_cols), bf16),
            jax.ShapeDtypeStruct((BASIS, 2 * BASIS), f32),
            jax.ShapeDtypeStruct((BASIS, 2 * BASIS), f32),
        ),
        in_specs=[SMEM, SMEM, ANY, ANY, ANY],
        out_specs=(VMEM, VMEM, VMEM),
        scratch_shapes=[
            pltpu.VMEM((levels, tile_rows, tile_cols), bf16),
            pltpu.VMEM((tile_cols, 2 * BASIS), bf16),
            pltpu.VMEM(rounded.shape, f32),
            pltpu.VMEM((third_cols // 128, levels, tile_rows, 128), f32),
            pltpu.VMEM((levels // 2, BASIS, 2 * BASIS), f32),
            pltpu.SemaphoreType.DMA((3,)),
        ],
        name="first",
    )(offset, level_index, tile_in, jnp.asarray(cols_twice), jnp.asarray(rounded))

    strips = [averaged] + [exchange(averaged, mask_of(0, k, 0)) for k in range(1, row_count)]
    selected = pl.pallas_call(
        functools.partial(select_kernel, full_rows),
        out_shape=jax.ShapeDtypeStruct((tile_rows, levels * third_cols), bf16),
        in_specs=[SMEM] + [VMEM] * row_count,
        out_specs=VMEM,
        name="select",
    )(offset, *strips)
    block_0 = exchange(selected, mask_of(3, 0, 0))
    block_1 = exchange(block_0, mask_of(1, 0, 0))
    block_2 = exchange(selected, mask_of(1, 0, 0))

    tile, spread, weights, target = pl.pallas_call(
        functools.partial(prepare_kernel, full_rows, amplitude, groups, col_count),
        out_shape=(
            jax.ShapeDtypeStruct(tile_in.shape, bf16),
            jax.ShapeDtypeStruct((4 * BASIS, tile_cols), bf16),
            jax.ShapeDtypeStruct((tile_rows, BASIS), f32),
            jax.ShapeDtypeStruct((levels // 2, BASIS, 2 * BASIS), f32),
        ),
        in_specs=[ANY, SMEM, ANY, ANY, ANY, ANY, ANY],
        out_specs=(VMEM,) * 4,
        scratch_shapes=[
            pltpu.VMEM((child_rows.shape[0] + parent_rows.shape[0], BASIS), f32),
            pltpu.VMEM(driving.shape, f32),
            pltpu.SemaphoreType.DMA((8,)),
        ],
        name="prepare",
    )(
        keep, offset, tile_in, jnp.asarray(spread_table), jnp.asarray(child_rows),
        jnp.asarray(parent_rows), driving,
    )

    mine = keep + exchange(send, flip)
    for mask in rounds:
        mine = mine + exchange(mine, mask)
    other = exchange(mine, flip)

    result = pl.pallas_call(
        functools.partial(final_kernel, full_rows, groups),
        out_shape=jax.ShapeDtypeStruct(tile_in.shape, bf16),
        in_specs=[SMEM, SMEM, SMEM] + [VMEM] * 9,
        out_specs=ANY,
        scratch_shapes=[
            pltpu.VMEM((levels // 2, BASIS, 2 * BASIS), f32),
            pltpu.VMEM((levels * tile_rows, 4 * BASIS), bf16),
            pltpu.VMEM(tile_in.shape, f32),
            pltpu.VMEM(tile_in.shape, bf16),
            pltpu.SemaphoreType.DMA((levels,)),
        ],
        name="final",
    )(
        offset, level_index, nudge_rate, mine, other, tile, spread, weights, target, block_0,
        block_1, block_2,
    )
    return result[None]


def solution(mesh):
    placed = (P("grp", None, "row", "col"), P(), P(), P(), P())
    sizes = tuple(mesh.shape[axis] for axis in AXES)
    return jax.shard_map(
        functools.partial(per_device, sizes),
        mesh=mesh,
        in_specs=placed,
        out_specs=P("grp", None, "row", "col"),
        check_vma=False,
    )
```

```python
import functools
import math

import jax
import jax.numpy as jnp
import numpy as np
from jax import lax
from jax.experimental import pallas as pl
from jax.experimental.pallas import tpu as pltpu
from jax.sharding import PartitionSpec as P

MAX_WAVE = 32
BASIS = 2 * MAX_WAVE
AXES = ("grp", "row", "col")
VMEM = pl.BlockSpec(memory_space=pltpu.VMEM)
SMEM = pl.BlockSpec(memory_space=pltpu.SMEM)
ANY = pl.BlockSpec(memory_space=pl.ANY)


def basis_table(positions, cell_count):
    period = 3 * cell_count
    orders = np.arange(1, MAX_WAVE + 1)
    angles = (np.asarray(positions)[:, None] * orders % period) * (2.0 * math.pi / period)
    scale = math.sqrt(2.0 / cell_count)
    constant = np.full((len(positions), 1), 1.0 / math.sqrt(cell_count))
    table = np.concatenate([constant, scale * np.cos(angles), scale * np.sin(angles[:, :-1])], 1)
    return table.astype(np.float32)


def halves(table):
    high = table.astype(jnp.bfloat16)
    return high, (table - high.astype(np.float32)).astype(jnp.bfloat16)


def split(value):
    high = value.astype(jnp.bfloat16)
    return high, (value - high.astype(jnp.float32)).astype(jnp.bfloat16)


def dot(a, b, contract=((1,), (0,))):
    return lax.dot_general(a, b, (contract, ((), ())), preferred_element_type=jnp.float32)


def parity_of_device():
    bits = lax.axis_index("grp") ^ lax.axis_index("row") ^ lax.axis_index("col")
    for shift in (8, 4, 2, 1):
        bits = bits ^ (bits >> shift)
    return bits & 1


def inverse_of(level_ref, parent_level, levels):
    found = jnp.int32(0)
    for level in range(levels):
        found = found + jnp.where(level_ref[level] == parent_level, level, 0)
    return found


def first_kernel(
    full_rows, amplitude, groups, columns, offset, level_index, tile_hbm, cols_hbm, rows_hbm,
    spread_hbm, child_rows_hbm, parent_rows_hbm, driving_hbm,
    averaged, keep, send, tile, spread, weights, target,
    cols, rows, sums, coeffs, turn_rows, driving, sems,
):
    levels, tile_rows, tile_cols = tile.shape
    third_rows, third_cols = tile_rows // 3, tile_cols // 3
    group, row, col = (lax.axis_index(a) for a in AXES)
    is_parent = group == groups - 1
    child_count = child_rows_hbm.shape[0]
    slot = jnp.where(is_parent, (groups - 1) * columns + col, col * (groups - 1) + group)
    copies = [
        pltpu.make_async_copy(tile_hbm, tile, sems.at[0]),
        pltpu.make_async_copy(cols_hbm.at[col], cols, sems.at[1]),
        pltpu.make_async_copy(rows_hbm, rows, sems.at[2]),
    ]
    later = [
        pltpu.make_async_copy(
            spread_hbm.at[slot, part // 2], spread.at[pl.ds(part * BASIS, BASIS)], sems.at[3 + part]
        )
        for part in range(4)
    ] + [
        pltpu.make_async_copy(driving_hbm, driving, sems.at[7]),
        pltpu.make_async_copy(child_rows_hbm, turn_rows.at[pl.ds(0, child_count)], sems.at[8]),
        pltpu.make_async_copy(
            parent_rows_hbm,
            turn_rows.at[pl.ds(child_count, parent_rows_hbm.shape[0])],
            sems.at[9],
        ),
    ]
    for copy in copies + later:
        copy.start()
    shift = offset[0]
    lanes = sums.shape[-1]
    depth = 3 * lanes
    cell = lax.broadcasted_iota(jnp.int32, (depth, lanes), 0)
    block = 3 * lax.broadcasted_iota(jnp.int32, (depth, lanes), 1)
    pick = jnp.where((cell >= block) & (cell < block + 3), 1.0, 0.0).astype(jnp.bfloat16)
    for copy in copies:
        copy.wait()

    def project(blocks, table, weights):
        left = lax.broadcasted_iota(jnp.int32, table.shape, 1) < BASIS
        zero = jnp.zeros_like(table)
        first, second = jnp.where(left, table, zero), jnp.where(left, zero, table)
        for pair in range(levels // 2):
            projected = dot(blocks[2 * pair], first) + dot(blocks[2 * pair + 1], second)
            high, low = split(projected)
            rows_first = ((0,), (0,))
            coeffs[pair] = dot(weights, high, rows_first) + dot(weights, low, rows_first)

    @pl.when(jnp.logical_not(is_parent))
    def _():
        flat = tile[...].reshape(levels * tile_rows, tile_cols)
        for part in range(third_cols // lanes):
            piece = dot(flat[:, part * depth : (part + 1) * depth], pick)
            sums[part] = piece.reshape(levels, tile_rows, lanes)
        blocks = []
        for parent_level in range(levels):
            level = inverse_of(level_index, parent_level, levels)
            totals = [
                sum(sums[part, level, pl.ds(a, third_rows, 3), :] for a in range(3))
                for part in range(third_cols // lanes)
            ]
            block = (jnp.concatenate(totals, axis=1) * (1.0 / 9.0)).astype(jnp.bfloat16)
            averaged[:, parent_level * third_cols : (parent_level + 1) * third_cols] = block
            blocks.append(block)
        table = cols[pl.ds(pl.multiple_of(group * third_cols, third_cols), third_cols), :]
        start = lax.rem(row * third_rows + shift, full_rows)
        project(blocks, table, rows[pl.ds(start, third_rows), :].astype(jnp.bfloat16))

    @pl.when(is_parent)
    def _():
        averaged[...] = jnp.zeros_like(averaged)
        cell = lax.broadcasted_iota(jnp.int32, (tile_rows, BASIS), 0)
        strip = lax.rem(row * tile_rows + cell - shift + full_rows, full_rows)
        weights = rows[pl.ds(pl.multiple_of(row * tile_rows, 8), tile_rows), :]
        weights = jnp.where(strip < full_rows // 3, 0.0, weights).astype(jnp.bfloat16)
        project([tile[level] for level in range(levels)], cols[...], weights)

    half = parity_of_device()
    keep[...] = coeffs[half]
    send[...] = coeffs[1 - half]
    for copy in later:
        copy.wait()
    period = 3 * full_rows
    child_start = lax.rem(3 * shift + row * tile_rows - 1 + period, period)
    start = jnp.where(is_parent, child_count + row * tile_rows, child_start)
    weights[...] = turn_rows[pl.ds(start, tile_rows), :]
    for pair in range(levels // 2):
        target[pair] = amplitude * jnp.concatenate(
            [driving[2 * pair], driving[2 * pair + 1]], axis=1
        )


def select_kernel(full_rows, third_rows, offset, first, second, out):
    tile_rows = out.shape[0]
    row = lax.axis_index("row")
    shape = (tile_rows, first.shape[0] + second.shape[0])
    cell = lax.broadcasted_iota(jnp.int32, shape, 0)
    wanted = lax.rem(row * tile_rows + cell - offset[0] + full_rows, full_rows)
    place = lax.broadcasted_iota(jnp.int32, shape, 1)
    held = (row ^ (place // third_rows)) * third_rows + place % third_rows
    pick = jnp.where(wanted == held, 1.0, 0.0).astype(jnp.bfloat16)
    strip = jnp.concatenate([first[...], second[...]], axis=0)
    out[...] = dot(pick, strip).astype(jnp.bfloat16)


def final_kernel(
    full_rows, groups, offset, level_index, rate, mine, other, tile, spread, weights, target,
    block_0, block_1, block_2, out_hbm, deficit, left, base, result, sems,
):
    levels, tile_rows, tile_cols = base.shape
    third_cols = tile_cols // 3
    group, row = lax.axis_index("grp"), lax.axis_index("row")
    is_parent = group == groups - 1
    half = parity_of_device()
    deficit[half] = target[half] - mine[...]
    deficit[1 - half] = target[1 - half] - other[...]
    is_left = lax.broadcasted_iota(jnp.int32, (tile_rows, 2 * BASIS), 1) < BASIS
    for pair in range(levels // 2):
        turned = jnp.dot(
            weights[...], deficit[pair], precision=lax.Precision.HIGHEST,
            preferred_element_type=jnp.float32,
        )
        for side in range(2):
            parent_level = 2 * pair + side
            high, low = split(turned * rate[parent_level])
            low = pltpu.roll(low.astype(jnp.float32), BASIS, 1).astype(jnp.bfloat16)
            here = is_left if side == 0 else ~is_left
            span = pl.ds(parent_level * tile_rows, tile_rows)
            left[span, : 2 * BASIS] = jnp.where(here, high, low)
            left[span, 2 * BASIS :] = jnp.where(here, high, jnp.zeros_like(high))
    increment = dot(left[...], spread[...])

    @pl.when(is_parent)
    def _():
        cell = lax.broadcasted_iota(jnp.int32, (tile_rows, third_cols), 0)
        strip = lax.rem(row * tile_rows + cell - offset[0] + full_rows, full_rows)
        covered = strip < full_rows // 3
        for level in range(levels):
            for third, block in enumerate((block_0, block_1, block_2)):
                span = slice(third * third_cols, (third + 1) * third_cols)
                arrived = block[:, level * third_cols : (level + 1) * third_cols]
                base[level, :, span] = jnp.where(
                    covered, arrived.astype(jnp.float32), tile[level, :, span].astype(jnp.float32)
                )

    @pl.when(jnp.logical_not(is_parent))
    def _():
        base[...] = tile[...].astype(jnp.float32)

    copies = []
    for parent_level in range(levels):
        level = jnp.where(is_parent, parent_level, inverse_of(level_index, parent_level, levels))
        rows = increment[parent_level * tile_rows : (parent_level + 1) * tile_rows]
        result[level] = (base[level] + rows).astype(jnp.bfloat16)
        copy = pltpu.make_async_copy(
            result.at[level], out_hbm.at[level], sems.at[parent_level]
        )
        copy.start()
        copies.append(copy)
    for copy in copies:
        copy.wait()


def per_device(sizes, fields, offset, level_index, nudge_rate, driving):
    groups, row_count, col_count = sizes
    tile_in = fields[0]
    levels, tile_rows, tile_cols = tile_in.shape
    third_rows, third_cols = tile_rows // 3, tile_cols // 3
    full_rows, full_cols = row_count * tile_rows, col_count * tile_cols
    f32, bf16 = jnp.float32, jnp.bfloat16

    cols = basis_table(3 * np.arange(full_cols), full_cols)
    cols_twice = np.concatenate([cols, cols], 1).reshape(col_count, tile_cols, 2 * BASIS)
    cols_twice = cols_twice.astype(bf16)
    parent_rows = basis_table(3 * np.arange(full_rows), full_rows)
    rounded = parent_rows.astype(bf16).astype(np.float32)
    rounded = np.concatenate([rounded, rounded[:third_rows]], 0)
    child_rows = basis_table(np.arange(3 * full_rows), full_rows)
    child_rows = np.concatenate([child_rows, child_rows[:tile_rows]], 0)
    child_cols = basis_table((np.arange(3 * full_cols) - 1) % (3 * full_cols), full_cols)
    spread_rows = np.concatenate([child_cols, cols], 0).reshape(-1, tile_cols, BASIS)
    spread_rows = spread_rows.transpose(0, 2, 1)
    spread_table = np.stack(halves(spread_rows), 1)
    amplitude = math.sqrt(full_rows * full_cols) / BASIS

    def mask_of(group_bits, row_bits, col_bits):
        return (group_bits * row_count + row_bits) * col_count + col_bits

    def exchange(value, mask):
        count = groups * row_count * col_count
        return lax.ppermute(value, AXES, [(i, i ^ mask) for i in range(count)])

    flip = mask_of(1, 0, 0)
    rounds = [mask_of(1 << k, 0, 0) ^ flip for k in range(1, groups.bit_length() - 1)]
    rounds += [mask_of(0, 0, 1 << k) ^ flip for k in range(col_count.bit_length() - 1)]
    rounds += [mask_of(0, 1 << k, 0) ^ flip for k in range(row_count.bit_length() - 1)]

    averaged, keep, send, tile, spread, weights, target = pl.pallas_call(
        functools.partial(first_kernel, full_rows, amplitude, groups, col_count),
        out_shape=(
            pltpu.VMEM((third_rows, levels * third_cols), bf16),
            pltpu.VMEM((BASIS, 2 * BASIS), f32),
            pltpu.VMEM((BASIS, 2 * BASIS), f32),
            pltpu.VMEM(tile_in.shape, bf16),
            pltpu.VMEM((4 * BASIS, tile_cols), bf16),
            pltpu.VMEM((tile_rows, BASIS), f32),
            pltpu.VMEM((levels // 2, BASIS, 2 * BASIS), f32),
        ),
        in_specs=[SMEM, SMEM] + [ANY] * 7,
        out_specs=(VMEM,) * 7,
        scratch_shapes=[
            pltpu.VMEM((tile_cols, 2 * BASIS), bf16),
            pltpu.VMEM(rounded.shape, f32),
            pltpu.VMEM((third_cols // 128, levels, tile_rows, 128), f32),
            pltpu.VMEM((levels // 2, BASIS, 2 * BASIS), f32),
            pltpu.VMEM((child_rows.shape[0] + parent_rows.shape[0], BASIS), f32),
            pltpu.VMEM(driving.shape, f32),
            pltpu.SemaphoreType.DMA((10,)),
        ],
        name="first",
    )(
        offset, level_index, tile_in, jnp.asarray(cols_twice), jnp.asarray(rounded),
        jnp.asarray(spread_table), jnp.asarray(child_rows), jnp.asarray(parent_rows), driving,
    )

    mine = keep + exchange(send, flip)
    for mask in rounds:
        mine = mine + exchange(mine, mask)
    other = exchange(mine, flip)

    strips = [averaged]
    for k in range(row_count.bit_length() - 1):
        held = strips[0] if k == 0 else jnp.concatenate(strips, 0)
        strips = [held, exchange(held, mask_of(0, 1 << k, 0))]
    selected = pl.pallas_call(
        functools.partial(select_kernel, full_rows, third_rows),
        out_shape=pltpu.VMEM((tile_rows, levels * third_cols), bf16),
        in_specs=[SMEM, VMEM, VMEM],
        out_specs=VMEM,
        name="select",
    )(offset, *(pltpu.with_memory_space_constraint(strip, pltpu.VMEM) for strip in strips))
    block_0 = exchange(selected, mask_of(3, 0, 0))
    block_2 = exchange(selected, mask_of(1, 0, 0))
    block_1 = exchange(block_0, mask_of(1, 0, 0))

    result = pl.pallas_call(
        functools.partial(final_kernel, full_rows, groups),
        out_shape=jax.ShapeDtypeStruct(tile_in.shape, bf16),
        in_specs=[SMEM, SMEM, SMEM] + [VMEM] * 9,
        out_specs=ANY,
        scratch_shapes=[
            pltpu.VMEM((levels // 2, BASIS, 2 * BASIS), f32),
            pltpu.VMEM((levels * tile_rows, 4 * BASIS), bf16),
            pltpu.VMEM(tile_in.shape, f32),
            pltpu.VMEM(tile_in.shape, bf16),
            pltpu.SemaphoreType.DMA((levels,)),
        ],
        name="final",
    )(
        offset, level_index, nudge_rate,
        *(
            pltpu.with_memory_space_constraint(value, pltpu.VMEM)
            for value in (mine, other, tile, spread, weights, target, block_0, block_1, block_2)
        ),
    )
    return result[None]


def solution(mesh):
    placed = (P("grp", None, "row", "col"), P(), P(), P(), P())
    sizes = tuple(mesh.shape[axis] for axis in AXES)
    return jax.shard_map(
        functools.partial(per_device, sizes),
        mesh=mesh,
        in_specs=placed,
        out_specs=P("grp", None, "row", "col"),
        check_vma=False,
    )
```

```python
import functools
import math

import jax
import jax.numpy as jnp
import numpy as np
from jax import lax
from jax.experimental import pallas as pl
from jax.experimental.pallas import tpu as pltpu
from jax.sharding import PartitionSpec as P

MAX_WAVE = 32
BASIS = 2 * MAX_WAVE
AXES = ("grp", "row", "col")
VMEM = pl.BlockSpec(memory_space=pltpu.VMEM)
SMEM = pl.BlockSpec(memory_space=pltpu.SMEM)
ANY = pl.BlockSpec(memory_space=pl.ANY)


def in_vmem(value):
    return pltpu.with_memory_space_constraint(value, pltpu.VMEM)


def in_hbm(value):
    return pltpu.with_memory_space_constraint(value, pltpu.HBM)


def basis_table(positions, cell_count):
    period = 3 * cell_count
    orders = np.arange(1, MAX_WAVE + 1)
    angles = (np.asarray(positions)[:, None] * orders % period) * (2.0 * math.pi / period)
    scale = math.sqrt(2.0 / cell_count)
    constant = np.full((len(positions), 1), 1.0 / math.sqrt(cell_count))
    table = np.concatenate([constant, scale * np.cos(angles), scale * np.sin(angles[:, :-1])], 1)
    return table.astype(np.float32)


def halves(table):
    high = table.astype(jnp.bfloat16)
    return high, (table - high.astype(np.float32)).astype(jnp.bfloat16)


def split(value):
    high = value.astype(jnp.bfloat16)
    return high, (value - high.astype(jnp.float32)).astype(jnp.bfloat16)


def dot(a, b, contract=((1,), (0,))):
    return lax.dot_general(a, b, (contract, ((), ())), preferred_element_type=jnp.float32)


def parity_of_device():
    bits = lax.axis_index("grp") ^ lax.axis_index("row") ^ lax.axis_index("col")
    for shift in (8, 4, 2, 1):
        bits = bits ^ (bits >> shift)
    return bits & 1


def inverse_of(level_ref, parent_level, levels):
    found = jnp.int32(0)
    for level in range(levels):
        found = found + jnp.where(level_ref[level] == parent_level, level, 0)
    return found


def first_kernel(
    full_rows, amplitude, groups, columns, tile_hbm, cols_hbm, rows_hbm, offset_hbm, level_hbm,
    rate_hbm, spread_hbm, child_rows_hbm, parent_rows_hbm, driving_hbm,
    averaged, keep, send, tile, spread, weights, target, whole_out, rate,
    cols, rows, sums, coeffs, turn_rows, driving, offset, level_index, sems,
):
    levels, tile_rows, tile_cols = tile.shape
    third_rows, third_cols = tile_rows // 3, tile_cols // 3
    group, row, col = (lax.axis_index(a) for a in AXES)
    is_parent = group == groups - 1
    child_count = child_rows_hbm.shape[0]
    slot = jnp.where(is_parent, (groups - 1) * columns + col, col * (groups - 1) + group)
    copies = [
        pltpu.make_async_copy(tile_hbm, tile, sems.at[0]),
        pltpu.make_async_copy(cols_hbm.at[col], cols, sems.at[1]),
        pltpu.make_async_copy(rows_hbm, rows, sems.at[2]),
        pltpu.make_async_copy(offset_hbm, offset, sems.at[10]),
        pltpu.make_async_copy(level_hbm, level_index, sems.at[11]),
    ]
    later = [
        pltpu.make_async_copy(
            spread_hbm.at[slot, part // 2], spread.at[pl.ds(part * BASIS, BASIS)], sems.at[3 + part]
        )
        for part in range(4)
    ] + [
        pltpu.make_async_copy(driving_hbm, driving, sems.at[7]),
        pltpu.make_async_copy(child_rows_hbm, turn_rows.at[pl.ds(0, child_count)], sems.at[8]),
        pltpu.make_async_copy(
            parent_rows_hbm,
            turn_rows.at[pl.ds(child_count, parent_rows_hbm.shape[0])],
            sems.at[9],
        ),
        pltpu.make_async_copy(rate_hbm, rate, sems.at[12]),
    ]
    for copy in copies + later:
        copy.start()
    lanes = sums.shape[-1]
    depth = 3 * lanes
    cell = lax.broadcasted_iota(jnp.int32, (depth, lanes), 0)
    block = 3 * lax.broadcasted_iota(jnp.int32, (depth, lanes), 1)
    pick = jnp.where((cell >= block) & (cell < block + 3), 1.0, 0.0).astype(jnp.bfloat16)
    for copy in copies:
        copy.wait()
    shift = offset[0]

    def project(blocks, table, weights):
        left = lax.broadcasted_iota(jnp.int32, table.shape, 1) < BASIS
        zero = jnp.zeros_like(table)
        first, second = jnp.where(left, table, zero), jnp.where(left, zero, table)
        for pair in range(levels // 2):
            projected = dot(blocks[2 * pair], first) + dot(blocks[2 * pair + 1], second)
            high, low = split(projected)
            rows_first = ((0,), (0,))
            coeffs[pair] = dot(weights, high, rows_first) + dot(weights, low, rows_first)

    @pl.when(jnp.logical_not(is_parent))
    def _():
        flat = tile[...].reshape(levels * tile_rows, tile_cols)
        for part in range(third_cols // lanes):
            piece = dot(flat[:, part * depth : (part + 1) * depth], pick)
            sums[part] = piece.reshape(levels, tile_rows, lanes)
        blocks = []
        for parent_level in range(levels):
            level = inverse_of(level_index, parent_level, levels)
            totals = [
                sum(sums[part, level, pl.ds(a, third_rows, 3), :] for a in range(3))
                for part in range(third_cols // lanes)
            ]
            block = (jnp.concatenate(totals, axis=1) * (1.0 / 9.0)).astype(jnp.bfloat16)
            averaged[:, parent_level * third_cols : (parent_level + 1) * third_cols] = block
            blocks.append(block)
        table = cols[pl.ds(pl.multiple_of(group * third_cols, third_cols), third_cols), :]
        start = lax.rem(row * third_rows + shift, full_rows)
        project(blocks, table, rows[pl.ds(start, third_rows), :].astype(jnp.bfloat16))

    @pl.when(is_parent)
    def _():
        averaged[...] = jnp.zeros_like(averaged)
        cell = lax.broadcasted_iota(jnp.int32, (tile_rows, BASIS), 0)
        strip = lax.rem(row * tile_rows + cell - shift + full_rows, full_rows)
        weights = rows[pl.ds(pl.multiple_of(row * tile_rows, 8), tile_rows), :]
        weights = jnp.where(strip < full_rows // 3, 0.0, weights).astype(jnp.bfloat16)
        project([tile[level] for level in range(levels)], cols[...], weights)

    whole_out[0] = shift
    for parent_level in range(levels):
        found = inverse_of(level_index, parent_level, levels)
        whole_out[1 + parent_level] = jnp.where(is_parent, parent_level, found)
    half = parity_of_device()
    keep[...] = coeffs[half]
    send[...] = coeffs[1 - half]
    for copy in later:
        copy.wait()
    period = 3 * full_rows
    child_start = lax.rem(3 * shift + row * tile_rows - 1 + period, period)
    start = jnp.where(is_parent, child_count + row * tile_rows, child_start)
    weights[...] = turn_rows[pl.ds(start, tile_rows), :]
    for pair in range(levels // 2):
        target[pair] = amplitude * jnp.concatenate(
            [driving[2 * pair], driving[2 * pair + 1]], axis=1
        )


def select_kernel(full_rows, third_rows, offset, first, second, out):
    tile_rows = out.shape[0]
    row = lax.axis_index("row")
    shape = (tile_rows, first.shape[0] + second.shape[0])
    cell = lax.broadcasted_iota(jnp.int32, shape, 0)
    wanted = lax.rem(row * tile_rows + cell - offset[0] + full_rows, full_rows)
    place = lax.broadcasted_iota(jnp.int32, shape, 1)
    held = (row ^ (place // third_rows)) * third_rows + place % third_rows
    pick = jnp.where(wanted == held, 1.0, 0.0).astype(jnp.bfloat16)
    strip = jnp.concatenate([first[...], second[...]], axis=0)
    out[...] = dot(pick, strip).astype(jnp.bfloat16)


def final_kernel(
    full_rows, groups, own_half, whole, rate, *refs,
):
    coeffs, tile, spread, weights, target, block_0, block_1, block_2 = refs[:8]
    if own_half:
        result, left, base = refs[8:]
    else:
        earlier, out_hbm, left, base, result, sems = refs[8:]
    _, tile_rows, tile_cols = tile.shape
    third_cols = tile_cols // 3
    group, row = lax.axis_index("grp"), lax.axis_index("row")
    is_parent = group == groups - 1
    half = parity_of_device()
    pair = half if own_half else 1 - half
    copies = []

    def write(source, pair):
        for side in range(2):
            target_level = out_hbm.at[whole[1 + 2 * pair + side]]
            copies.append(
                pltpu.make_async_copy(source.at[side], target_level, sems.at[len(copies)])
            )
            copies[-1].start()

    if not own_half:
        write(earlier, half)
    is_left = lax.broadcasted_iota(jnp.int32, (tile_rows, 2 * BASIS), 1) < BASIS
    turned = jnp.dot(
        weights[...], target[pair] - coeffs[...], precision=lax.Precision.HIGHEST,
        preferred_element_type=jnp.float32,
    )
    for side in range(2):
        high, low = split(turned * rate[2 * pair + side])
        low = pltpu.roll(low.astype(jnp.float32), BASIS, 1).astype(jnp.bfloat16)
        here = is_left if side == 0 else ~is_left
        span = pl.ds(side * tile_rows, tile_rows)
        left[span, : 2 * BASIS] = jnp.where(here, high, low)
        left[span, 2 * BASIS :] = jnp.where(here, high, jnp.zeros_like(high))
    increment = dot(left[...], spread[...])

    @pl.when(is_parent)
    def _():
        cell = lax.broadcasted_iota(jnp.int32, (tile_rows, third_cols), 0)
        strip = lax.rem(row * tile_rows + cell - whole[0] + full_rows, full_rows)
        covered = strip < full_rows // 3
        for side in range(2):
            level = 2 * pair + side
            for third, block in enumerate((block_0, block_1, block_2)):
                span = slice(third * third_cols, (third + 1) * third_cols)
                arrived = block[:, pl.ds(pl.multiple_of(level * third_cols, 128), third_cols)]
                base[side, :, span] = jnp.where(
                    covered, arrived.astype(jnp.float32), tile[level, :, span].astype(jnp.float32)
                )

    levels_out = [whole[1 + 2 * pair + side] for side in range(2)]

    @pl.when(jnp.logical_not(is_parent))
    def _():
        for side in range(2):
            base[side] = tile[levels_out[side]].astype(jnp.float32)

    for side in range(2):
        rows = increment[side * tile_rows : (side + 1) * tile_rows]
        result[side] = (base[side] + rows).astype(jnp.bfloat16)
    if not own_half:
        write(result, pair)
    for copy in copies:
        copy.wait()


def per_device(sizes, fields, offset, level_index, nudge_rate, driving):
    groups, row_count, col_count = sizes
    tile_in = fields[0]
    levels, tile_rows, tile_cols = tile_in.shape
    third_rows, third_cols = tile_rows // 3, tile_cols // 3
    full_rows, full_cols = row_count * tile_rows, col_count * tile_cols
    f32, bf16 = jnp.float32, jnp.bfloat16

    cols = basis_table(3 * np.arange(full_cols), full_cols)
    cols_twice = np.concatenate([cols, cols], 1).reshape(col_count, tile_cols, 2 * BASIS)
    cols_twice = cols_twice.astype(bf16)
    parent_rows = basis_table(3 * np.arange(full_rows), full_rows)
    rounded = parent_rows.astype(bf16).astype(np.float32)
    rounded = np.concatenate([rounded, rounded[:third_rows]], 0)
    child_rows = basis_table(np.arange(3 * full_rows), full_rows)
    child_rows = np.concatenate([child_rows, child_rows[:tile_rows]], 0)
    child_cols = basis_table((np.arange(3 * full_cols) - 1) % (3 * full_cols), full_cols)
    spread_rows = np.concatenate([child_cols, cols], 0).reshape(-1, tile_cols, BASIS)
    spread_rows = spread_rows.transpose(0, 2, 1)
    spread_table = np.stack(halves(spread_rows), 1)
    amplitude = math.sqrt(full_rows * full_cols) / BASIS

    def mask_of(group_bits, row_bits, col_bits):
        return (group_bits * row_count + row_bits) * col_count + col_bits

    def exchange(value, masks):
        even, odd = masks if isinstance(masks, tuple) else (masks, masks)
        count = groups * row_count * col_count
        pairs = [(i, i ^ (odd if i.bit_count() % 2 else even)) for i in range(count)]
        return lax.ppermute(value, AXES, pairs)

    flip = mask_of(1, 0, 0)
    across = [mask_of(1 << k, 0, 0) ^ flip for k in range(1, groups.bit_length() - 1)]
    across += [mask_of(0, 0, 1 << k) ^ flip for k in range(col_count.bit_length() - 1)]
    along = [mask_of(0, 1 << k, 0) ^ flip for k in range(row_count.bit_length() - 1)]
    rounds = []
    while across and along:
        one, two = across.pop(0), along.pop(0)
        rounds += [(one, two), (two, one)]
    rounds += [(mask, mask) for mask in across + along]

    averaged, keep, send, tile, spread, weights, target, whole, rate = pl.pallas_call(
        functools.partial(first_kernel, full_rows, amplitude, groups, col_count),
        out_shape=(
            pltpu.VMEM((third_rows, levels * third_cols), bf16),
            pltpu.VMEM((BASIS, 2 * BASIS), f32),
            pltpu.VMEM((BASIS, 2 * BASIS), f32),
            pltpu.VMEM(tile_in.shape, bf16),
            pltpu.VMEM((4 * BASIS, tile_cols), bf16),
            pltpu.VMEM((tile_rows, BASIS), f32),
            pltpu.VMEM((levels // 2, BASIS, 2 * BASIS), f32),
            pltpu.SMEM((1 + levels,), jnp.int32),
            pltpu.SMEM((levels,), f32),
        ),
        in_specs=[ANY] * 10,
        out_specs=(VMEM,) * 7 + (SMEM, SMEM),
        scratch_shapes=[
            pltpu.VMEM((tile_cols, 2 * BASIS), bf16),
            pltpu.VMEM(rounded.shape, f32),
            pltpu.VMEM((third_cols // 128, levels, tile_rows, 128), f32),
            pltpu.VMEM((levels // 2, BASIS, 2 * BASIS), f32),
            pltpu.VMEM((child_rows.shape[0] + parent_rows.shape[0], BASIS), f32),
            pltpu.VMEM(driving.shape, f32),
            pltpu.SMEM((1,), jnp.int32),
            pltpu.SMEM((levels,), jnp.int32),
            pltpu.SemaphoreType.DMA((13,)),
        ],
        name="first",
    )(
        tile_in, jnp.asarray(cols_twice), jnp.asarray(rounded), offset,
        in_hbm(level_index), in_hbm(nudge_rate),
        jnp.asarray(spread_table), jnp.asarray(child_rows), jnp.asarray(parent_rows), driving,
    )

    mine = keep + exchange(send, flip)
    for masks in rounds:
        mine = mine + exchange(mine, masks)
    other = exchange(mine, flip)

    strips = [averaged]
    for k in range(row_count.bit_length() - 1):
        held = strips[0] if k == 0 else jnp.concatenate(strips, 0)
        strips = [held, exchange(held, mask_of(0, 1 << k, 0))]
    selected = pl.pallas_call(
        functools.partial(select_kernel, full_rows, third_rows),
        out_shape=pltpu.VMEM((tile_rows, levels * third_cols), bf16),
        in_specs=[SMEM, VMEM, VMEM],
        out_specs=VMEM,
        name="select",
    )(whole, *(in_vmem(strip) for strip in strips))
    block_0 = exchange(selected, mask_of(3, 0, 0))
    block_2 = exchange(selected, mask_of(1, 0, 0))
    block_1 = exchange(block_0, mask_of(1, 0, 0))

    def finish(coeffs, earlier):
        two_levels = (2, tile_rows, tile_cols)
        scratch = [pltpu.VMEM((2 * tile_rows, 4 * BASIS), bf16), pltpu.VMEM(two_levels, f32)]
        if earlier:
            scratch += [pltpu.VMEM(two_levels, bf16), pltpu.SemaphoreType.DMA((4,))]
            out_shape, out_spec = jax.ShapeDtypeStruct(tile_in.shape, bf16), ANY
        else:
            out_shape, out_spec = pltpu.VMEM(two_levels, bf16), VMEM
        values = (coeffs, tile, spread, weights, target, block_0, block_1, block_2, *earlier)
        return pl.pallas_call(
            functools.partial(final_kernel, full_rows, groups, not earlier),
            out_shape=out_shape,
            in_specs=[SMEM, SMEM] + [VMEM] * len(values),
            out_specs=out_spec,
            scratch_shapes=scratch,
        )(whole, rate, *(in_vmem(value) for value in values))

    partly = finish(mine, ())
    return finish(other, (partly,))[None]


def solution(mesh):
    placed = (P("grp", None, "row", "col"), P(), P(), P(), P())
    sizes = tuple(mesh.shape[axis] for axis in AXES)
    return jax.shard_map(
        functools.partial(per_device, sizes),
        mesh=mesh,
        in_specs=placed,
        out_specs=P("grp", None, "row", "col"),
        check_vma=False,
    )
```

```python
import functools
import math

import jax
import jax.numpy as jnp
import numpy as np
from jax import lax
from jax.experimental import pallas as pl
from jax.experimental.pallas import tpu as pltpu
from jax.sharding import PartitionSpec as P

MAX_WAVE = 32
BASIS = 2 * MAX_WAVE
AXES = ("grp", "row", "col")
VMEM = pl.BlockSpec(memory_space=pltpu.VMEM)
SMEM = pl.BlockSpec(memory_space=pltpu.SMEM)
ANY = pl.BlockSpec(memory_space=pl.ANY)


def in_vmem(value):
    return pltpu.with_memory_space_constraint(value, pltpu.VMEM)


def in_hbm(value):
    return pltpu.with_memory_space_constraint(value, pltpu.HBM)


def basis_table(positions, cell_count):
    period = 3 * cell_count
    orders = np.arange(1, MAX_WAVE + 1)
    angles = (np.asarray(positions)[:, None] * orders % period) * (2.0 * math.pi / period)
    scale = math.sqrt(2.0 / cell_count)
    constant = np.full((len(positions), 1), 1.0 / math.sqrt(cell_count))
    table = np.concatenate([constant, scale * np.cos(angles), scale * np.sin(angles[:, :-1])], 1)
    return table.astype(np.float32)


def halves(table):
    high = table.astype(jnp.bfloat16)
    return high, (table - high.astype(np.float32)).astype(jnp.bfloat16)


def split(value):
    high = value.astype(jnp.bfloat16)
    return high, (value - high.astype(jnp.float32)).astype(jnp.bfloat16)


def dot(a, b, contract=((1,), (0,))):
    return lax.dot_general(a, b, (contract, ((), ())), preferred_element_type=jnp.float32)


def parity_of_device():
    bits = lax.axis_index("grp") ^ lax.axis_index("row") ^ lax.axis_index("col")
    for shift in (8, 4, 2, 1):
        bits = bits ^ (bits >> shift)
    return bits & 1


def inverse_of(level_ref, parent_level, levels):
    found = jnp.int32(0)
    for level in range(levels):
        found = found + jnp.where(level_ref[level] == parent_level, level, 0)
    return found


def first_kernel(
    groups, columns, tile_hbm, cols_hbm, level_hbm, rate_hbm, rows_hbm, spread_hbm,
    turns_hbm, driving_hbm,
    averaged, keep, send, tile, spread, target, rows, turns, places, rate,
    cols, sums, projected, driving, level_index, sems,
):
    levels, tile_rows, tile_cols = tile.shape
    third_rows, third_cols = tile_rows // 3, tile_cols // 3
    group, _, col = (lax.axis_index(a) for a in AXES)
    is_parent = group == groups - 1
    slot = jnp.where(is_parent, (groups - 1) * columns + col, col * (groups - 1) + group)
    copies = [
        pltpu.make_async_copy(tile_hbm, tile, sems.at[0]),
        pltpu.make_async_copy(cols_hbm.at[col], cols, sems.at[1]),
        pltpu.make_async_copy(level_hbm, level_index, sems.at[2]),
    ]
    later = [
        pltpu.make_async_copy(
            spread_hbm.at[slot, part // 2], spread.at[pl.ds(part * BASIS, BASIS)], sems.at[3 + part]
        )
        for part in range(4)
    ] + [
        pltpu.make_async_copy(driving_hbm, driving, sems.at[7]),
        pltpu.make_async_copy(turns_hbm, turns, sems.at[8]),
        pltpu.make_async_copy(rows_hbm, rows, sems.at[9]),
        pltpu.make_async_copy(rate_hbm, rate, sems.at[10]),
    ]
    for copy in copies + later:
        copy.start()
    lanes = sums.shape[-1]
    depth = 3 * lanes
    cell = lax.broadcasted_iota(jnp.int32, (depth, lanes), 0)
    block = 3 * lax.broadcasted_iota(jnp.int32, (depth, lanes), 1)
    pick = jnp.where((cell >= block) & (cell < block + 3), 1.0, 0.0).astype(jnp.bfloat16)
    for copy in copies:
        copy.wait()

    def project(blocks, table):
        left = lax.broadcasted_iota(jnp.int32, table.shape, 1) < BASIS
        zero = jnp.zeros_like(table)
        first, second = jnp.where(left, table, zero), jnp.where(left, zero, table)
        for pair in range(levels // 2):
            span = pl.ds(0, blocks[0].shape[0])
            projected[pair, span] = dot(blocks[2 * pair], first) + dot(blocks[2 * pair + 1], second)

    @pl.when(jnp.logical_not(is_parent))
    def _():
        flat = tile[...].reshape(levels * tile_rows, tile_cols)
        for part in range(third_cols // lanes):
            piece = dot(flat[:, part * depth : (part + 1) * depth], pick)
            sums[part] = piece.reshape(levels, tile_rows, lanes)
        blocks = []
        for parent_level in range(levels):
            level = inverse_of(level_index, parent_level, levels)
            totals = [
                sum(sums[part, level, pl.ds(a, third_rows, 3), :] for a in range(3))
                for part in range(third_cols // lanes)
            ]
            block = (jnp.concatenate(totals, axis=1) * (1.0 / 9.0)).astype(jnp.bfloat16)
            averaged[:, parent_level * third_cols : (parent_level + 1) * third_cols] = block
            blocks.append(block)
        projected[...] = jnp.zeros_like(projected)
        table = cols[pl.ds(pl.multiple_of(group * third_cols, third_cols), third_cols), :]
        project(blocks, table)

    @pl.when(is_parent)
    def _():
        averaged[...] = jnp.zeros_like(averaged)
        project([tile[level] for level in range(levels)], cols[...])

    half = parity_of_device()
    keep[...] = projected[half]
    send[...] = projected[1 - half]
    for parent_level in range(levels):
        found = inverse_of(level_index, parent_level, levels)
        places[parent_level] = jnp.where(is_parent, parent_level, found)
    for copy in later:
        copy.wait()
    for pair in range(levels // 2):
        target[pair] = jnp.concatenate([driving[2 * pair], driving[2 * pair + 1]], axis=1)


def coeffs_kernel(full_rows, groups, offset, mine, partner, rows, out):
    tile_rows = mine.shape[0]
    group, row = lax.axis_index("grp"), lax.axis_index("row")
    shift = offset[0]
    cell = lax.broadcasted_iota(jnp.int32, (tile_rows, BASIS), 0)
    strip = lax.rem(row * tile_rows + cell - shift + full_rows, full_rows)
    strip_start = lax.rem(row * (tile_rows // 3) + shift, full_rows)

    def weights(is_parent):
        start = jnp.where(is_parent, row * tile_rows, strip_start)
        counted = jnp.where(is_parent, strip - full_rows // 3, tile_rows // 3 - 1 - cell) >= 0
        return jnp.where(counted, rows[pl.ds(start, tile_rows), :], 0.0).astype(jnp.bfloat16)

    table = jnp.concatenate([weights(group == groups - 1), weights((group ^ 1) == groups - 1)], 0)
    high, low = split(jnp.concatenate([mine[...], partner[...]], axis=0))
    out[...] = dot(table, high, ((0,), (0,))) + dot(table, low, ((0,), (0,)))


def select_kernel(full_rows, groups, exchanges, offset, first, second, turns, out, weights):
    tile_rows = out.shape[0]
    third_rows = tile_rows // 3
    row = lax.axis_index("row")
    is_parent = lax.axis_index("grp") == groups - 1
    shape = (tile_rows, first.shape[0] + second.shape[0])
    cell = lax.broadcasted_iota(jnp.int32, shape, 0)
    wanted = lax.rem(row * tile_rows + cell - offset[0] + full_rows, full_rows)
    place = lax.broadcasted_iota(jnp.int32, shape, 1)
    block = place // third_rows
    source = jnp.zeros_like(block)
    for step in range(exchanges):
        source = source + ((block >> step) & 1) * (1 << (exchanges - 1 - step))
    held = (row ^ source) * third_rows + place % third_rows
    pick = jnp.where(wanted == held, 1.0, 0.0).astype(jnp.bfloat16)
    strip = jnp.concatenate([first[...], second[...]], axis=0)
    out[...] = dot(pick, strip).astype(jnp.bfloat16)
    period = 3 * full_rows
    child_start = lax.rem(3 * offset[0] + row * tile_rows - 1 + period, period)
    start = jnp.where(is_parent, period + tile_rows + row * tile_rows, child_start)
    weights[...] = turns[pl.ds(start, tile_rows), :]


def final_kernel(
    full_rows, groups, amplitude, own_half, offset, places, rate, *refs,
):
    coeffs, tile, spread, weights, target, block_0, block_1, block_2 = refs[:8]
    if own_half:
        result, left, base = refs[8:]
    else:
        earlier, out_hbm, left, base, result, sems = refs[8:]
    _, tile_rows, tile_cols = tile.shape
    third_cols = tile_cols // 3
    group, row = lax.axis_index("grp"), lax.axis_index("row")
    is_parent = group == groups - 1
    half = parity_of_device()
    pair = half if own_half else 1 - half
    copies = []

    def write(source, pair):
        for side in range(2):
            target_level = out_hbm.at[places[2 * pair + side]]
            copies.append(
                pltpu.make_async_copy(source.at[side], target_level, sems.at[len(copies)])
            )
            copies[-1].start()

    if not own_half:
        write(earlier, half)
    is_left = lax.broadcasted_iota(jnp.int32, (tile_rows, 2 * BASIS), 1) < BASIS
    turned = jnp.dot(
        weights[...], amplitude * target[pair] - coeffs[...], precision=lax.Precision.HIGHEST,
        preferred_element_type=jnp.float32,
    )
    for side in range(2):
        high, low = split(turned * rate[2 * pair + side])
        low = pltpu.roll(low.astype(jnp.float32), BASIS, 1).astype(jnp.bfloat16)
        here = is_left if side == 0 else ~is_left
        span = pl.ds(side * tile_rows, tile_rows)
        left[span, : 2 * BASIS] = jnp.where(here, high, low)
        left[span, 2 * BASIS :] = jnp.where(here, high, jnp.zeros_like(high))
    increment = dot(left[...], spread[...])

    @pl.when(is_parent)
    def _():
        cell = lax.broadcasted_iota(jnp.int32, (tile_rows, third_cols), 0)
        strip = lax.rem(row * tile_rows + cell - offset[0] + full_rows, full_rows)
        covered = strip < full_rows // 3
        for side in range(2):
            level = 2 * pair + side
            for third, block in enumerate((block_0, block_1, block_2)):
                span = slice(third * third_cols, (third + 1) * third_cols)
                arrived = block[:, pl.ds(pl.multiple_of(level * third_cols, 128), third_cols)]
                base[side, :, span] = jnp.where(
                    covered, arrived.astype(jnp.float32), tile[level, :, span].astype(jnp.float32)
                )

    levels_out = [places[2 * pair + side] for side in range(2)]

    @pl.when(jnp.logical_not(is_parent))
    def _():
        for side in range(2):
            base[side] = tile[levels_out[side]].astype(jnp.float32)

    for side in range(2):
        rows = increment[side * tile_rows : (side + 1) * tile_rows]
        result[side] = (base[side] + rows).astype(jnp.bfloat16)
    if not own_half:
        write(result, pair)
    for copy in copies:
        copy.wait()


def per_device(sizes, fields, offset, level_index, nudge_rate, driving):
    groups, row_count, col_count = sizes
    tile_in = fields[0]
    levels, tile_rows, tile_cols = tile_in.shape
    third_rows, third_cols = tile_rows // 3, tile_cols // 3
    full_rows, full_cols = row_count * tile_rows, col_count * tile_cols
    f32, bf16 = jnp.float32, jnp.bfloat16

    cols = basis_table(3 * np.arange(full_cols), full_cols)
    cols_twice = np.concatenate([cols, cols], 1).reshape(col_count, tile_cols, 2 * BASIS)
    cols_twice = cols_twice.astype(bf16)
    parent_rows = basis_table(3 * np.arange(full_rows), full_rows)
    rounded = parent_rows.astype(bf16).astype(np.float32)
    rounded = np.concatenate([rounded, rounded[:tile_rows]], 0)
    child_rows = basis_table(np.arange(3 * full_rows), full_rows)
    turns = np.concatenate([child_rows, child_rows[:tile_rows], parent_rows], 0)
    child_cols = basis_table((np.arange(3 * full_cols) - 1) % (3 * full_cols), full_cols)
    spread_rows = np.concatenate([child_cols, cols], 0).reshape(-1, tile_cols, BASIS)
    spread_rows = spread_rows.transpose(0, 2, 1)
    spread_table = np.stack(halves(spread_rows), 1)
    amplitude = math.sqrt(full_rows * full_cols) / BASIS

    def mask_of(group_bits, row_bits, col_bits):
        return (group_bits * row_count + row_bits) * col_count + col_bits

    def exchange(value, mask):
        count = groups * row_count * col_count
        return lax.ppermute(value, AXES, [(i, i ^ mask) for i in range(count)])

    flip = mask_of(1, 0, 0)
    across = [mask_of(1 << k, 0, 0) ^ flip for k in range(1, groups.bit_length() - 1)]
    across += [mask_of(0, 0, 1 << k) ^ flip for k in range(col_count.bit_length() - 1)]
    row_bits = [1 << k for k in reversed(range(row_count.bit_length() - 1))]
    along = [mask_of(0, bit, 0) ^ flip for bit in row_bits]
    rounds = across + along[::-1]

    averaged, keep, send, tile, spread, target, rows, turns, places, rate = pl.pallas_call(
        functools.partial(first_kernel, groups, col_count),
        out_shape=(
            pltpu.VMEM((third_rows, levels * third_cols), bf16),
            pltpu.VMEM((tile_rows, 2 * BASIS), f32),
            pltpu.VMEM((tile_rows, 2 * BASIS), f32),
            pltpu.VMEM(tile_in.shape, bf16),
            pltpu.VMEM((4 * BASIS, tile_cols), bf16),
            pltpu.VMEM((levels // 2, BASIS, 2 * BASIS), f32),
            pltpu.VMEM(rounded.shape, f32),
            pltpu.VMEM(turns.shape, f32),
            pltpu.SMEM((levels,), jnp.int32),
            pltpu.SMEM((levels,), f32),
        ),
        in_specs=[ANY] * 8,
        out_specs=(VMEM,) * 8 + (SMEM, SMEM),
        scratch_shapes=[
            pltpu.VMEM((tile_cols, 2 * BASIS), bf16),
            pltpu.VMEM((third_cols // 128, levels, tile_rows, 128), f32),
            pltpu.VMEM((levels // 2, tile_rows, 2 * BASIS), f32),
            pltpu.VMEM(driving.shape, f32),
            pltpu.SMEM((levels,), jnp.int32),
            pltpu.SemaphoreType.DMA((11,)),
        ],
        name="first",
    )(
        tile_in, jnp.asarray(cols_twice), in_hbm(level_index), in_hbm(nudge_rate),
        jnp.asarray(rounded), jnp.asarray(spread_table), jnp.asarray(turns), driving,
    )

    partner = exchange(send, flip)
    mine = pl.pallas_call(
        functools.partial(coeffs_kernel, full_rows, groups),
        out_shape=pltpu.VMEM((BASIS, 2 * BASIS), f32),
        in_specs=[SMEM, VMEM, VMEM, VMEM],
        out_specs=VMEM,
        name="coeffs",
    )(offset, in_vmem(keep), in_vmem(partner), in_vmem(rows))
    for mask in rounds:
        mine = mine + exchange(mine, mask)
    other = exchange(mine, flip)

    strips = [averaged]
    for step, bit in enumerate(row_bits):
        held = strips[0] if step == 0 else jnp.concatenate(strips, 0)
        strips = [held, exchange(held, mask_of(0, bit, 0))]
    selected, weights = pl.pallas_call(
        functools.partial(select_kernel, full_rows, groups, len(row_bits)),
        out_shape=(
            pltpu.VMEM((tile_rows, levels * third_cols), bf16),
            pltpu.VMEM((tile_rows, BASIS), f32),
        ),
        in_specs=[SMEM, VMEM, VMEM, VMEM],
        out_specs=(VMEM, VMEM),
        name="select",
    )(offset, *(in_vmem(value) for value in (*strips, turns)))
    block_0 = exchange(selected, mask_of(3, 0, 0))
    block_2 = exchange(selected, mask_of(1, 0, 0))
    block_1 = exchange(block_0, mask_of(1, 0, 0))

    def finish(coeffs, earlier):
        two_levels = (2, tile_rows, tile_cols)
        scratch = [pltpu.VMEM((2 * tile_rows, 4 * BASIS), bf16), pltpu.VMEM(two_levels, f32)]
        if earlier:
            scratch += [pltpu.VMEM(two_levels, bf16), pltpu.SemaphoreType.DMA((4,))]
            out_shape, out_spec = jax.ShapeDtypeStruct(tile_in.shape, bf16), ANY
        else:
            out_shape, out_spec = pltpu.VMEM(two_levels, bf16), VMEM
        values = (coeffs, tile, spread, weights, target, block_0, block_1, block_2, *earlier)
        return pl.pallas_call(
            functools.partial(final_kernel, full_rows, groups, amplitude, not earlier),
            out_shape=out_shape,
            in_specs=[SMEM] * 3 + [VMEM] * len(values),
            out_specs=out_spec,
            scratch_shapes=scratch,
        )(offset, places, rate, *(in_vmem(value) for value in values))

    partly = finish(mine, ())
    return finish(other, (partly,))[None]


def solution(mesh):
    placed = (P("grp", None, "row", "col"), P(), P(), P(), P())
    sizes = tuple(mesh.shape[axis] for axis in AXES)
    return jax.shard_map(
        functools.partial(per_device, sizes),
        mesh=mesh,
        in_specs=placed,
        out_specs=P("grp", None, "row", "col"),
        check_vma=False,
    )
```

```python
import functools
import math

import jax
import jax.numpy as jnp
import numpy as np
from jax import lax
from jax.experimental import pallas as pl
from jax.experimental.pallas import tpu as pltpu
from jax.sharding import PartitionSpec as P

MAX_WAVE = 32
BASIS = 2 * MAX_WAVE
AXES = ("grp", "row", "col")
VMEM = pl.BlockSpec(memory_space=pltpu.VMEM)
SMEM = pl.BlockSpec(memory_space=pltpu.SMEM)
ANY = pl.BlockSpec(memory_space=pl.ANY)


def in_vmem(value):
    return pltpu.with_memory_space_constraint(value, pltpu.VMEM)


def in_hbm(value):
    return pltpu.with_memory_space_constraint(value, pltpu.HBM)


def basis_table(positions, cell_count):
    period = 3 * cell_count
    orders = np.arange(1, MAX_WAVE + 1)
    angles = (np.asarray(positions)[:, None] * orders % period) * (2.0 * math.pi / period)
    scale = math.sqrt(2.0 / cell_count)
    constant = np.full((len(positions), 1), 1.0 / math.sqrt(cell_count))
    table = np.concatenate([constant, scale * np.cos(angles), scale * np.sin(angles[:, :-1])], 1)
    return table.astype(np.float32)


def halves(table):
    high = table.astype(jnp.bfloat16)
    return high, (table - high.astype(np.float32)).astype(jnp.bfloat16)


def split(value):
    high = value.astype(jnp.bfloat16)
    return high, (value - high.astype(jnp.float32)).astype(jnp.bfloat16)


def dot(a, b, contract=((1,), (0,))):
    return lax.dot_general(a, b, (contract, ((), ())), preferred_element_type=jnp.float32)


def parity_of_device():
    bits = lax.axis_index("grp") ^ lax.axis_index("row") ^ lax.axis_index("col")
    for shift in (8, 4, 2, 1):
        bits = bits ^ (bits >> shift)
    return bits & 1


def inverse_of(level_ref, parent_level, levels):
    found = jnp.int32(0)
    for level in range(levels):
        found = found + jnp.where(level_ref[level] == parent_level, level, 0)
    return found


def first_kernel(
    groups, columns, tile_hbm, cols_hbm, level_hbm, rate_hbm, spread_hbm, rows_hbm,
    averaged, keep, send, tile, spread, rows, places, rate,
    cols, sums, projected, level_index, sems,
):
    levels, tile_rows, tile_cols = tile.shape
    third_rows, third_cols = tile_rows // 3, tile_cols // 3
    group, _, col = (lax.axis_index(a) for a in AXES)
    is_parent = group == groups - 1
    slot = jnp.where(is_parent, (groups - 1) * columns + col, col * (groups - 1) + group)
    own_third = pl.ds(pl.multiple_of(group * third_cols, third_cols), third_cols)
    own_cols = pltpu.make_async_copy(
        cols_hbm.at[col, own_third], cols.at[pl.ds(0, third_cols)], sems.at[1]
    )
    all_cols = pltpu.make_async_copy(cols_hbm.at[col], cols, sems.at[1])
    copies = [
        pltpu.make_async_copy(tile_hbm, tile, sems.at[0]),
        pltpu.make_async_copy(level_hbm, level_index, sems.at[2]),
    ]
    later = [
        pltpu.make_async_copy(spread_hbm.at[slot], spread, sems.at[3]),
        pltpu.make_async_copy(rows_hbm, rows, sems.at[4]),
        pltpu.make_async_copy(rate_hbm, rate, sems.at[6]),
    ]
    for copy in copies:
        copy.start()
    pl.when(is_parent)(all_cols.start)
    pl.when(jnp.logical_not(is_parent))(own_cols.start)
    for copy in later:
        copy.start()
    lanes = sums.shape[-1]
    depth = 3 * lanes
    cell = lax.broadcasted_iota(jnp.int32, (depth, lanes), 0)
    block = 3 * lax.broadcasted_iota(jnp.int32, (depth, lanes), 1)
    pick = jnp.where((cell >= block) & (cell < block + 3), 1.0, 0.0).astype(jnp.bfloat16)
    for copy in copies:
        copy.wait()

    def project(blocks, table):
        left = lax.broadcasted_iota(jnp.int32, table.shape, 1) < BASIS
        zero = jnp.zeros_like(table)
        first, second = jnp.where(left, table, zero), jnp.where(left, zero, table)
        for pair in range(levels // 2):
            span = pl.ds(0, blocks[0].shape[0])
            projected[pair, span] = dot(blocks[2 * pair], first) + dot(blocks[2 * pair + 1], second)

    @pl.when(jnp.logical_not(is_parent))
    def _():
        flat = tile[...].reshape(levels * tile_rows, tile_cols)
        for part in range(third_cols // lanes):
            piece = dot(flat[:, part * depth : (part + 1) * depth], pick)
            sums[part] = piece.reshape(levels, tile_rows, lanes)
        blocks = []
        for parent_level in range(levels):
            level = inverse_of(level_index, parent_level, levels)
            totals = [
                sum(sums[part, level, pl.ds(a, third_rows, 3), :] for a in range(3))
                for part in range(third_cols // lanes)
            ]
            block = (jnp.concatenate(totals, axis=1) * (1.0 / 9.0)).astype(jnp.bfloat16)
            averaged[:, parent_level * third_cols : (parent_level + 1) * third_cols] = block
            blocks.append(block)
        projected[...] = jnp.zeros_like(projected)
        own_cols.wait()
        project(blocks, cols[pl.ds(0, third_cols), :])

    @pl.when(is_parent)
    def _():
        averaged[...] = jnp.zeros_like(averaged)
        all_cols.wait()
        project([tile[level] for level in range(levels)], cols[...])

    half = parity_of_device()
    keep[...] = projected[half]
    send[...] = projected[1 - half]
    for parent_level in range(levels):
        found = inverse_of(level_index, parent_level, levels)
        places[parent_level] = jnp.where(is_parent, parent_level, found)
    for copy in later:
        copy.wait()


def coeffs_kernel(full_rows, groups, offset, mine, partner, rows, out):
    tile_rows = mine.shape[0]
    group, row = lax.axis_index("grp"), lax.axis_index("row")
    shift = offset[0]
    cell = lax.broadcasted_iota(jnp.int32, (tile_rows, BASIS), 0)
    strip = lax.rem(row * tile_rows + cell - shift + full_rows, full_rows)
    strip_start = lax.rem(row * (tile_rows // 3) + shift, full_rows)

    def weights(is_parent):
        start = jnp.where(is_parent, row * tile_rows, strip_start)
        counted = jnp.where(is_parent, strip - full_rows // 3, tile_rows // 3 - 1 - cell) >= 0
        return jnp.where(counted, rows[pl.ds(start, tile_rows), :][:, :BASIS], 0.0).astype(
            jnp.bfloat16
        )

    table = jnp.concatenate([weights(group == groups - 1), weights((group ^ 1) == groups - 1)], 0)
    high, low = split(jnp.concatenate([mine[...], partner[...]], axis=0))
    out[...] = dot(table, high, ((0,), (0,))) + dot(table, low, ((0,), (0,)))


def select_kernel(
    full_rows, groups, exchanges, amplitude, offset, first, second, rows, driving, out, weights, target,
):
    tile_rows = out.shape[0]
    third_rows = tile_rows // 3
    row = lax.axis_index("row")
    is_parent = lax.axis_index("grp") == groups - 1
    shape = (tile_rows, first.shape[0] + second.shape[0])
    cell = lax.broadcasted_iota(jnp.int32, shape, 0)
    wanted = lax.rem(row * tile_rows + cell - offset[0] + full_rows, full_rows)
    place = lax.broadcasted_iota(jnp.int32, shape, 1)
    block = place // third_rows
    source = jnp.zeros_like(block)
    for step in range(exchanges):
        source = source + ((block >> step) & 1) * (1 << (exchanges - 1 - step))
    held = (row ^ source) * third_rows + place % third_rows
    pick = jnp.where(wanted == held, 1.0, 0.0).astype(jnp.bfloat16)
    strip = jnp.concatenate([first[...], second[...]], axis=0)
    out[...] = dot(pick, strip).astype(jnp.bfloat16)
    period = 3 * full_rows
    child_start = lax.rem(3 * offset[0] + row * tile_rows - 1 + period, period)
    own = pl.ds(pl.multiple_of(full_rows + (row + 1) * tile_rows, 8), tile_rows)
    high, low = split(
        jnp.where(
            is_parent, rows[own, :][:, :BASIS], rows[pl.ds(child_start, tile_rows), :][:, BASIS:]
        )
    )
    weights[...] = jnp.concatenate([high, low, high], axis=1)
    for pair in range(target.shape[0]):
        both = [driving[2 * pair], driving[2 * pair + 1]]
        target[pair] = amplitude * jnp.concatenate(both, axis=1)


def final_kernel(full_rows, groups, own_half, offset, places, rate, *refs):
    coeffs, spread, weights, target = refs[:4]
    group, row = lax.axis_index("grp"), lax.axis_index("row")
    is_parent = group == groups - 1
    half = parity_of_device()
    pair = half if own_half else 1 - half
    if own_half:
        tile, block_0, block_1, block_2, result, later_base, left, base = refs[4:]
    else:
        earlier, base, out_hbm, left, result, sems = refs[4:]
    _, tile_rows, tile_cols = base.shape
    third_cols = tile_cols // 3
    copies = []

    def write(source, side, pair):
        place = out_hbm.at[places[2 * pair + side]]
        copies.append(pltpu.make_async_copy(source.at[side], place, sems.at[len(copies)]))
        copies[-1].start()

    if not own_half:
        write(earlier, 0, half)
        write(earlier, 1, half)
    high, low = split(target[pair] - coeffs[...])
    turned = dot(weights[...], jnp.concatenate([high, high, low], axis=0))
    is_left = lax.broadcasted_iota(jnp.int32, (tile_rows, 2 * BASIS), 1) < BASIS
    for side in range(2):
        high, low = split(turned * rate[2 * pair + side])
        low = pltpu.roll(low.astype(jnp.float32), BASIS, 1).astype(jnp.bfloat16)
        here = is_left if side == 0 else ~is_left
        span = pl.ds(side * tile_rows, tile_rows)
        left[span, : 2 * BASIS] = jnp.where(here, high, low)
        left[span, 2 * BASIS :] = jnp.where(here, high, jnp.zeros_like(high))
    high, low = spread[0], spread[1]
    increment = dot(left[...], jnp.concatenate([high, high, low, low], axis=0))

    if own_half:

        @pl.when(is_parent)
        def _():
            cell = lax.broadcasted_iota(jnp.int32, (tile_rows, third_cols), 0)
            strip = lax.rem(row * tile_rows + cell - offset[0] + full_rows, full_rows)
            covered = strip < full_rows // 3
            for goal, goal_pair in ((base, half), (later_base, 1 - half)):
                for side in range(2):
                    level = 2 * goal_pair + side
                    for third, block in enumerate((block_0, block_1, block_2)):
                        span = slice(third * third_cols, (third + 1) * third_cols)
                        lanes = pl.ds(pl.multiple_of(level * third_cols, 128), third_cols)
                        arrived = block[:, lanes].astype(jnp.float32)
                        own = tile[level, :, span].astype(jnp.float32)
                        goal[side, :, span] = jnp.where(covered, arrived, own)

        @pl.when(jnp.logical_not(is_parent))
        def _():
            for goal, goal_pair in ((base, half), (later_base, 1 - half)):
                for side in range(2):
                    goal[side] = tile[places[2 * goal_pair + side]].astype(jnp.float32)

    for side in range(2):
        rows = increment[side * tile_rows : (side + 1) * tile_rows]
        result[side] = (base[side] + rows).astype(jnp.bfloat16)
        if not own_half:
            write(result, side, pair)
    for copy in copies:
        copy.wait()


def per_device(sizes, fields, offset, level_index, nudge_rate, driving):
    groups, row_count, col_count = sizes
    tile_in = fields[0]
    levels, tile_rows, tile_cols = tile_in.shape
    third_rows, third_cols = tile_rows // 3, tile_cols // 3
    full_rows, full_cols = row_count * tile_rows, col_count * tile_cols
    f32, bf16 = jnp.float32, jnp.bfloat16

    cols = basis_table(3 * np.arange(full_cols), full_cols)
    cols_twice = np.concatenate([cols, cols], 1).reshape(col_count, tile_cols, 2 * BASIS)
    cols_twice = cols_twice.astype(bf16)
    parent_rows = basis_table(3 * np.arange(full_rows), full_rows)
    rounded = parent_rows.astype(bf16).astype(np.float32)
    rounded = np.concatenate([rounded, rounded[:tile_rows]], 0)
    child_rows = basis_table(np.arange(3 * full_rows), full_rows)
    row_table = np.zeros((3 * full_rows + tile_rows, 2 * BASIS), np.float32)
    row_table[: 2 * full_rows + tile_rows, :BASIS] = np.concatenate([rounded, parent_rows], 0)
    row_table[:, BASIS:] = np.concatenate([child_rows, child_rows[:tile_rows]], 0)
    child_cols = basis_table((np.arange(3 * full_cols) - 1) % (3 * full_cols), full_cols)
    spread_rows = np.concatenate([child_cols, cols], 0).reshape(-1, tile_cols, BASIS)
    spread_rows = spread_rows.transpose(0, 2, 1)
    spread_table = np.stack(halves(spread_rows), 1)
    amplitude = math.sqrt(full_rows * full_cols) / BASIS

    def mask_of(group_bits, row_bits, col_bits):
        return (group_bits * row_count + row_bits) * col_count + col_bits

    def exchange(value, mask):
        count = groups * row_count * col_count
        return lax.ppermute(value, AXES, [(i, i ^ mask) for i in range(count)])

    flip = mask_of(1, 0, 0)
    across = [mask_of(1 << k, 0, 0) ^ flip for k in range(1, groups.bit_length() - 1)]
    across += [mask_of(0, 0, 1 << k) ^ flip for k in range(col_count.bit_length() - 1)]
    row_bits = [1 << k for k in reversed(range(row_count.bit_length() - 1))]
    along = [mask_of(0, bit, 0) ^ flip for bit in row_bits]
    rounds = across + along[::-1]

    averaged, keep, send, tile, spread, rows, places, rate = pl.pallas_call(
        functools.partial(first_kernel, groups, col_count),
        out_shape=(
            pltpu.VMEM((third_rows, levels * third_cols), bf16),
            pltpu.VMEM((tile_rows, 2 * BASIS), f32),
            pltpu.VMEM((tile_rows, 2 * BASIS), f32),
            pltpu.VMEM(tile_in.shape, bf16),
            pltpu.VMEM((2, BASIS, tile_cols), bf16),
            pltpu.VMEM(row_table.shape, f32),
            pltpu.SMEM((levels,), jnp.int32),
            pltpu.SMEM((levels,), f32),
        ),
        in_specs=[ANY] * 6,
        out_specs=(VMEM,) * 6 + (SMEM, SMEM),
        scratch_shapes=[
            pltpu.VMEM((tile_cols, 2 * BASIS), bf16),
            pltpu.VMEM((third_cols // 128, levels, tile_rows, 128), f32),
            pltpu.VMEM((levels // 2, tile_rows, 2 * BASIS), f32),
            pltpu.SMEM((levels,), jnp.int32),
            pltpu.SemaphoreType.DMA((7,)),
        ],
        name="first",
    )(
        tile_in, jnp.asarray(cols_twice), in_hbm(level_index), in_hbm(nudge_rate),
        jnp.asarray(spread_table), jnp.asarray(row_table),
    )

    partner = exchange(send, flip)
    mine = pl.pallas_call(
        functools.partial(coeffs_kernel, full_rows, groups),
        out_shape=pltpu.VMEM((BASIS, 2 * BASIS), f32),
        in_specs=[SMEM, VMEM, VMEM, VMEM],
        out_specs=VMEM,
        name="coeffs",
    )(offset, in_vmem(keep), in_vmem(partner), in_vmem(rows))
    for mask in rounds:
        mine = mine + exchange(mine, mask)
    other = exchange(mine, flip)

    strips = [averaged]
    for step, bit in enumerate(row_bits):
        held = strips[0] if step == 0 else jnp.concatenate(strips, 0)
        strips = [held, exchange(held, mask_of(0, bit, 0))]
    selected, weights, target = pl.pallas_call(
        functools.partial(select_kernel, full_rows, groups, len(row_bits), amplitude),
        out_shape=(
            pltpu.VMEM((tile_rows, levels * third_cols), bf16),
            pltpu.VMEM((tile_rows, 3 * BASIS), bf16),
            pltpu.VMEM((levels // 2, BASIS, 2 * BASIS), f32),
        ),
        in_specs=[SMEM] + [VMEM] * 4,
        out_specs=(VMEM,) * 3,
        name="select",
    )(offset, *(in_vmem(value) for value in (*strips, rows, driving)))
    block_0 = exchange(selected, mask_of(3, 0, 0))
    block_2 = exchange(selected, mask_of(1, 0, 0))
    block_1 = exchange(block_0, mask_of(1, 0, 0))

    def finish(name, coeffs, values, out_shape, out_spec, scratch):
        values = (coeffs, spread, weights, target, *values)
        return pl.pallas_call(
            functools.partial(final_kernel, full_rows, groups, name == "final_own"),
            out_shape=out_shape,
            in_specs=[SMEM] * 3 + [VMEM] * len(values),
            out_specs=out_spec,
            scratch_shapes=[pltpu.VMEM((2 * tile_rows, 4 * BASIS), bf16), *scratch],
        )(offset, places, rate, *(in_vmem(value) for value in values))

    two_levels = (2, tile_rows, tile_cols)
    earlier = finish(
        "final_own", mine, (tile, block_0, block_1, block_2),
        (pltpu.VMEM(two_levels, bf16), pltpu.VMEM(two_levels, f32)), (VMEM, VMEM),
        [pltpu.VMEM(two_levels, f32)],
    )
    result = finish(
        "final_other", other, earlier, jax.ShapeDtypeStruct(tile_in.shape, bf16), ANY,
        [pltpu.VMEM(two_levels, bf16), pltpu.SemaphoreType.DMA((4,))],
    )
    return result[None]


def solution(mesh):
    placed = (P("grp", None, "row", "col"), P(), P(), P(), P())
    sizes = tuple(mesh.shape[axis] for axis in AXES)
    return jax.shard_map(
        functools.partial(per_device, sizes),
        mesh=mesh,
        in_specs=placed,
        out_specs=P("grp", None, "row", "col"),
        check_vma=False,
    )
```

```python
import functools
import math

import jax
import jax.numpy as jnp
import numpy as np
from jax import lax
from jax.experimental import pallas as pl
from jax.experimental.pallas import tpu as pltpu
from jax.sharding import PartitionSpec as P

MAX_WAVE = 32
BASIS = 2 * MAX_WAVE
AXES = ("grp", "row", "col")
VMEM = pl.BlockSpec(memory_space=pltpu.VMEM)
SMEM = pl.BlockSpec(memory_space=pltpu.SMEM)
ANY = pl.BlockSpec(memory_space=pl.ANY)


def in_vmem(value):
    return pltpu.with_memory_space_constraint(value, pltpu.VMEM)


def in_hbm(value):
    return pltpu.with_memory_space_constraint(value, pltpu.HBM)


def basis_table(positions, cell_count):
    period = 3 * cell_count
    orders = np.arange(1, MAX_WAVE + 1)
    angles = (np.asarray(positions)[:, None] * orders % period) * (2.0 * math.pi / period)
    scale = math.sqrt(2.0 / cell_count)
    constant = np.full((len(positions), 1), 1.0 / math.sqrt(cell_count))
    table = np.concatenate([constant, scale * np.cos(angles), scale * np.sin(angles[:, :-1])], 1)
    return table.astype(np.float32)


def halves(table):
    high = table.astype(jnp.bfloat16)
    return high, (table - high.astype(np.float32)).astype(jnp.bfloat16)


def split(value):
    high = value.astype(jnp.bfloat16)
    return high, (value - high.astype(jnp.float32)).astype(jnp.bfloat16)


def dot(a, b, contract=((1,), (0,))):
    return lax.dot_general(a, b, (contract, ((), ())), preferred_element_type=jnp.float32)


def parity_of_device():
    bits = lax.axis_index("grp") ^ lax.axis_index("row") ^ lax.axis_index("col")
    for shift in (8, 4, 2, 1):
        bits = bits ^ (bits >> shift)
    return bits & 1


def inverse_of(level_ref, parent_level, levels):
    found = jnp.int32(0)
    for level in range(levels):
        found = found + jnp.where(level_ref[level] == parent_level, level, 0)
    return found


def first_kernel(
    groups, columns, tile_hbm, cols_hbm, level_hbm, rate_hbm, spread_hbm, rows_hbm,
    averaged, keep, send, tile, spread, rows, places, rate,
    cols, sums, projected, level_index, sems,
):
    levels, tile_rows, tile_cols = tile.shape
    third_rows, third_cols = tile_rows // 3, tile_cols // 3
    group, _, col = (lax.axis_index(a) for a in AXES)
    is_parent = group == groups - 1
    slot = jnp.where(is_parent, (groups - 1) * columns + col, col * (groups - 1) + group)
    own_third = pl.ds(pl.multiple_of(group * third_cols, third_cols), third_cols)
    own_cols = pltpu.make_async_copy(
        cols_hbm.at[col, own_third], cols.at[pl.ds(0, third_cols)], sems.at[1]
    )
    all_cols = pltpu.make_async_copy(cols_hbm.at[col], cols, sems.at[1])
    copies = [
        pltpu.make_async_copy(tile_hbm, tile, sems.at[0]),
        pltpu.make_async_copy(level_hbm, level_index, sems.at[2]),
    ]
    later = [
        pltpu.make_async_copy(spread_hbm.at[slot], spread, sems.at[3]),
        pltpu.make_async_copy(rows_hbm, rows, sems.at[4]),
        pltpu.make_async_copy(rate_hbm, rate, sems.at[6]),
    ]
    for copy in copies:
        copy.start()
    pl.when(is_parent)(all_cols.start)
    pl.when(jnp.logical_not(is_parent))(own_cols.start)
    for copy in later:
        copy.start()
    lanes = sums.shape[-1]
    depth = 3 * lanes
    cell = lax.broadcasted_iota(jnp.int32, (depth, lanes), 0)
    block = 3 * lax.broadcasted_iota(jnp.int32, (depth, lanes), 1)
    pick = jnp.where((cell >= block) & (cell < block + 3), 1.0, 0.0).astype(jnp.bfloat16)
    for copy in copies:
        copy.wait()

    def project(blocks, table):
        left = lax.broadcasted_iota(jnp.int32, table.shape, 1) < BASIS
        zero = jnp.zeros_like(table)
        first, second = jnp.where(left, table, zero), jnp.where(left, zero, table)
        for pair in range(levels // 2):
            span = pl.ds(0, blocks[0].shape[0])
            projected[pair, span] = dot(blocks[2 * pair], first) + dot(blocks[2 * pair + 1], second)

    @pl.when(jnp.logical_not(is_parent))
    def _():
        flat = tile[...].reshape(levels * tile_rows, tile_cols)
        for part in range(third_cols // lanes):
            piece = dot(flat[:, part * depth : (part + 1) * depth], pick)
            sums[part] = piece.reshape(levels, tile_rows, lanes)
        blocks = []
        for parent_level in range(levels):
            level = inverse_of(level_index, parent_level, levels)
            totals = [
                sum(sums[part, level, pl.ds(a, third_rows, 3), :] for a in range(3))
                for part in range(third_cols // lanes)
            ]
            block = (jnp.concatenate(totals, axis=1) * (1.0 / 9.0)).astype(jnp.bfloat16)
            averaged[:, parent_level * third_cols : (parent_level + 1) * third_cols] = block
            blocks.append(block)
        projected[...] = jnp.zeros_like(projected)
        own_cols.wait()
        project(blocks, cols[pl.ds(0, third_cols), :])

    @pl.when(is_parent)
    def _():
        averaged[...] = jnp.zeros_like(averaged)
        all_cols.wait()
        project([tile[level] for level in range(levels)], cols[...])

    half = parity_of_device()
    keep[...] = projected[half]
    send[...] = projected[1 - half]
    for parent_level in range(levels):
        found = inverse_of(level_index, parent_level, levels)
        places[parent_level] = jnp.where(is_parent, parent_level, found)
    for copy in later:
        copy.wait()


def coeffs_kernel(full_rows, groups, offset, mine, partner, rows, out):
    tile_rows = mine.shape[0]
    group, row = lax.axis_index("grp"), lax.axis_index("row")
    shift = offset[0]
    cell = lax.broadcasted_iota(jnp.int32, (tile_rows, BASIS), 0)
    strip = lax.rem(row * tile_rows + cell - shift + full_rows, full_rows)
    strip_start = lax.rem(row * (tile_rows // 3) + shift, full_rows)

    def weights(is_parent):
        start = jnp.where(is_parent, row * tile_rows, strip_start)
        counted = jnp.where(is_parent, strip - full_rows // 3, tile_rows // 3 - 1 - cell) >= 0
        return jnp.where(counted, rows[pl.ds(start, tile_rows), :][:, :BASIS], 0.0).astype(
            jnp.bfloat16
        )

    table = jnp.concatenate([weights(group == groups - 1), weights((group ^ 1) == groups - 1)], 0)
    high, low = split(jnp.concatenate([mine[...], partner[...]], axis=0))
    out[...] = dot(table, high, ((0,), (0,))) + dot(table, low, ((0,), (0,)))


def select_kernel(
    full_rows, groups, exchanges, amplitude, offset, first, second, rows, driving, out, weights, target,
):
    tile_rows = out.shape[0]
    third_rows = tile_rows // 3
    row = lax.axis_index("row")
    is_parent = lax.axis_index("grp") == groups - 1
    shape = (tile_rows, first.shape[0] + second.shape[0])
    cell = lax.broadcasted_iota(jnp.int32, shape, 0)
    wanted = lax.rem(row * tile_rows + cell - offset[0] + full_rows, full_rows)
    place = lax.broadcasted_iota(jnp.int32, shape, 1)
    block = place // third_rows
    source = jnp.zeros_like(block)
    for step in range(exchanges):
        source = source + ((block >> step) & 1) * (1 << (exchanges - 1 - step))
    held = (row ^ source) * third_rows + place % third_rows
    pick = jnp.where(wanted == held, 1.0, 0.0).astype(jnp.bfloat16)
    strip = jnp.concatenate([first[...], second[...]], axis=0)
    out[...] = dot(pick, strip).astype(jnp.bfloat16)
    period = 3 * full_rows
    child_start = lax.rem(3 * offset[0] + row * tile_rows - 1 + period, period)
    own = pl.ds(pl.multiple_of(full_rows + (row + 1) * tile_rows, 8), tile_rows)
    high, low = split(
        jnp.where(
            is_parent, rows[own, :][:, :BASIS], rows[pl.ds(child_start, tile_rows), :][:, BASIS:]
        )
    )
    weights[...] = jnp.concatenate([high, low, high], axis=1)
    for pair in range(target.shape[0]):
        both = [driving[2 * pair], driving[2 * pair + 1]]
        target[pair] = amplitude * jnp.concatenate(both, axis=1)


def final_kernel(full_rows, groups, own_half, offset, places, rate, *refs):
    coeffs, spread, weights, target = refs[:4]
    group, row = lax.axis_index("grp"), lax.axis_index("row")
    is_parent = group == groups - 1
    half = parity_of_device()
    pair = half if own_half else 1 - half
    if own_half:
        tile, block_0, block_1, block_2, result, later_base, left, base = refs[4:]
    else:
        earlier, base, out_hbm, left, result, sems = refs[4:]
    _, tile_rows, tile_cols = base.shape
    third_cols = tile_cols // 3
    copies = []

    def write(source, side, pair):
        place = out_hbm.at[places[2 * pair + side]]
        copies.append(pltpu.make_async_copy(source.at[side], place, sems.at[len(copies)]))
        copies[-1].start()

    if not own_half:
        write(earlier, 0, half)
        write(earlier, 1, half)
    high, low = split(target[pair] - coeffs[...])
    turned = dot(weights[...], jnp.concatenate([high, high, low], axis=0))
    is_left = lax.broadcasted_iota(jnp.int32, (tile_rows, 2 * BASIS), 1) < BASIS
    for side in range(2):
        high, low = split(turned * rate[2 * pair + side])
        low = pltpu.roll(low.astype(jnp.float32), BASIS, 1).astype(jnp.bfloat16)
        here = is_left if side == 0 else ~is_left
        span = pl.ds(side * tile_rows, tile_rows)
        left[span, : 2 * BASIS] = jnp.where(here, high, low)
        left[span, 2 * BASIS :] = jnp.where(here, high, jnp.zeros_like(high))
    high, low = spread[0], spread[1]
    increment = dot(left[...], jnp.concatenate([high, high, low, low], axis=0))

    if own_half:

        @pl.when(is_parent)
        def _():
            cell = lax.broadcasted_iota(jnp.int32, (tile_rows, third_cols), 0)
            strip = lax.rem(row * tile_rows + cell - offset[0] + full_rows, full_rows)
            covered = strip < full_rows // 3
            for goal, goal_pair in ((base, half), (later_base, 1 - half)):
                for side in range(2):
                    level = 2 * goal_pair + side
                    for third, block in enumerate((block_0, block_1, block_2)):
                        span = slice(third * third_cols, (third + 1) * third_cols)
                        lanes = pl.ds(pl.multiple_of(level * third_cols, 128), third_cols)
                        arrived = block[:, lanes].astype(jnp.float32)
                        own = tile[level, :, span].astype(jnp.float32)
                        goal[side, :, span] = jnp.where(covered, arrived, own)

        @pl.when(jnp.logical_not(is_parent))
        def _():
            for goal, goal_pair in ((base, half), (later_base, 1 - half)):
                for side in range(2):
                    goal[side] = tile[places[2 * goal_pair + side]].astype(jnp.float32)

    for side in range(2):
        rows = increment[side * tile_rows : (side + 1) * tile_rows]
        result[side] = (base[side] + rows).astype(jnp.bfloat16)
        if not own_half:
            write(result, side, pair)
    for copy in copies:
        copy.wait()


def per_device(sizes, fields, offset, level_index, nudge_rate, driving):
    groups, row_count, col_count = sizes
    tile_in = fields[0]
    levels, tile_rows, tile_cols = tile_in.shape
    third_rows, third_cols = tile_rows // 3, tile_cols // 3
    full_rows, full_cols = row_count * tile_rows, col_count * tile_cols
    f32, bf16 = jnp.float32, jnp.bfloat16

    cols = basis_table(3 * np.arange(full_cols), full_cols)
    cols_twice = np.concatenate([cols, cols], 1).reshape(col_count, tile_cols, 2 * BASIS)
    cols_twice = cols_twice.astype(bf16)
    parent_rows = basis_table(3 * np.arange(full_rows), full_rows)
    rounded = parent_rows.astype(bf16).astype(np.float32)
    rounded = np.concatenate([rounded, rounded[:tile_rows]], 0)
    child_rows = basis_table(np.arange(3 * full_rows), full_rows)
    row_table = np.zeros((3 * full_rows + tile_rows, 2 * BASIS), np.float32)
    row_table[: 2 * full_rows + tile_rows, :BASIS] = np.concatenate([rounded, parent_rows], 0)
    row_table[:, BASIS:] = np.concatenate([child_rows, child_rows[:tile_rows]], 0)
    child_cols = basis_table((np.arange(3 * full_cols) - 1) % (3 * full_cols), full_cols)
    spread_rows = np.concatenate([child_cols, cols], 0).reshape(-1, tile_cols, BASIS)
    spread_rows = spread_rows.transpose(0, 2, 1)
    spread_table = np.stack(halves(spread_rows), 1)
    amplitude = math.sqrt(full_rows * full_cols) / BASIS

    def mask_of(group_bits, row_bits, col_bits):
        return (group_bits * row_count + row_bits) * col_count + col_bits

    def exchange(value, mask, odd_mask=None):
        masks = (mask, mask if odd_mask is None else odd_mask)
        count = groups * row_count * col_count
        pairs = [(i, i ^ masks[i.bit_count() % 2]) for i in range(count)]
        return lax.ppermute(value, AXES, pairs)

    flip = mask_of(1, 0, 0)
    across = [mask_of(1 << k, 0, 0) ^ flip for k in range(1, groups.bit_length() - 1)]
    across += [mask_of(0, 0, 1 << k) ^ flip for k in range(col_count.bit_length() - 1)]
    row_bits = [1 << k for k in reversed(range(row_count.bit_length() - 1))]
    along = [mask_of(0, bit, 0) ^ flip for bit in row_bits]
    along = along[::-1]
    rounds = across + along
    odd_rounds = across[:1] + along[:1] + across[1:] + along[1:]

    averaged, keep, send, tile, spread, rows, places, rate = pl.pallas_call(
        functools.partial(first_kernel, groups, col_count),
        out_shape=(
            pltpu.VMEM((third_rows, levels * third_cols), bf16),
            pltpu.VMEM((tile_rows, 2 * BASIS), f32),
            pltpu.VMEM((tile_rows, 2 * BASIS), f32),
            pltpu.VMEM(tile_in.shape, bf16),
            pltpu.VMEM((2, BASIS, tile_cols), bf16),
            pltpu.VMEM(row_table.shape, f32),
            pltpu.SMEM((levels,), jnp.int32),
            pltpu.SMEM((levels,), f32),
        ),
        in_specs=[ANY] * 6,
        out_specs=(VMEM,) * 6 + (SMEM, SMEM),
        scratch_shapes=[
            pltpu.VMEM((tile_cols, 2 * BASIS), bf16),
            pltpu.VMEM((third_cols // 128, levels, tile_rows, 128), f32),
            pltpu.VMEM((levels // 2, tile_rows, 2 * BASIS), f32),
            pltpu.SMEM((levels,), jnp.int32),
            pltpu.SemaphoreType.DMA((7,)),
        ],
        name="first",
    )(
        tile_in, jnp.asarray(cols_twice), in_hbm(level_index), in_hbm(nudge_rate),
        jnp.asarray(spread_table), jnp.asarray(row_table),
    )

    partner = exchange(send, flip)
    mine = pl.pallas_call(
        functools.partial(coeffs_kernel, full_rows, groups),
        out_shape=pltpu.VMEM((BASIS, 2 * BASIS), f32),
        in_specs=[SMEM, VMEM, VMEM, VMEM],
        out_specs=VMEM,
        name="coeffs",
    )(offset, in_vmem(keep), in_vmem(partner), in_vmem(rows))
    for masks in zip(rounds, odd_rounds):
        mine = mine + exchange(mine, masks[0], masks[1])
    other = exchange(mine, flip)

    strips = [averaged]
    for step, bit in enumerate(row_bits):
        held = strips[0] if step == 0 else jnp.concatenate(strips, 0)
        strips = [held, exchange(held, mask_of(0, bit, 0))]
    selected, weights, target = pl.pallas_call(
        functools.partial(select_kernel, full_rows, groups, len(row_bits), amplitude),
        out_shape=(
            pltpu.VMEM((tile_rows, levels * third_cols), bf16),
            pltpu.VMEM((tile_rows, 3 * BASIS), bf16),
            pltpu.VMEM((levels // 2, BASIS, 2 * BASIS), f32),
        ),
        in_specs=[SMEM] + [VMEM] * 4,
        out_specs=(VMEM,) * 3,
        name="select",
    )(offset, *(in_vmem(value) for value in (*strips, rows, driving)))
    block_0 = exchange(selected, mask_of(3, 0, 0))
    block_2 = exchange(selected, mask_of(1, 0, 0))
    block_1 = exchange(block_0, mask_of(1, 0, 0))

    def finish(name, coeffs, values, out_shape, out_spec, scratch):
        values = (coeffs, spread, weights, target, *values)
        return pl.pallas_call(
            functools.partial(final_kernel, full_rows, groups, name == "final_own"),
            out_shape=out_shape,
            in_specs=[SMEM] * 3 + [VMEM] * len(values),
            out_specs=out_spec,
            scratch_shapes=[pltpu.VMEM((2 * tile_rows, 4 * BASIS), bf16), *scratch],
        )(offset, places, rate, *(in_vmem(value) for value in values))

    two_levels = (2, tile_rows, tile_cols)
    earlier = finish(
        "final_own", mine, (tile, block_0, block_1, block_2),
        (pltpu.VMEM(two_levels, bf16), pltpu.VMEM(two_levels, f32)), (VMEM, VMEM),
        [pltpu.VMEM(two_levels, f32)],
    )
    result = finish(
        "final_other", other, earlier, jax.ShapeDtypeStruct(tile_in.shape, bf16), ANY,
        [pltpu.VMEM(two_levels, bf16), pltpu.SemaphoreType.DMA((4,))],
    )
    return result[None]


def solution(mesh):
    placed = (P("grp", None, "row", "col"), P(), P(), P(), P())
    sizes = tuple(mesh.shape[axis] for axis in AXES)
    return jax.shard_map(
        functools.partial(per_device, sizes),
        mesh=mesh,
        in_specs=placed,
        out_specs=P("grp", None, "row", "col"),
        check_vma=False,
    )
```

```python
import functools
import math

import jax
import jax.numpy as jnp
import numpy as np
from jax import lax
from jax.experimental import pallas as pl
from jax.experimental.pallas import tpu as pltpu
from jax.sharding import PartitionSpec as P

MAX_WAVE = 32
BASIS = 2 * MAX_WAVE
AXES = ("grp", "row", "col")
VMEM = pl.BlockSpec(memory_space=pltpu.VMEM)
SMEM = pl.BlockSpec(memory_space=pltpu.SMEM)
ANY = pl.BlockSpec(memory_space=pl.ANY)


def in_vmem(value):
    return pltpu.with_memory_space_constraint(value, pltpu.VMEM)


def in_hbm(value):
    return pltpu.with_memory_space_constraint(value, pltpu.HBM)


def basis_table(positions, cell_count):
    period = 3 * cell_count
    orders = np.arange(1, MAX_WAVE + 1)
    angles = (np.asarray(positions)[:, None] * orders % period) * (2.0 * math.pi / period)
    scale = math.sqrt(2.0 / cell_count)
    constant = np.full((len(positions), 1), 1.0 / math.sqrt(cell_count))
    table = np.concatenate([constant, scale * np.cos(angles), scale * np.sin(angles[:, :-1])], 1)
    return table.astype(np.float32)


def halves(table):
    high = table.astype(jnp.bfloat16)
    return high, (table - high.astype(np.float32)).astype(jnp.bfloat16)


def split(value):
    high = value.astype(jnp.bfloat16)
    return high, (value - high.astype(jnp.float32)).astype(jnp.bfloat16)


def dot(a, b, contract=((1,), (0,))):
    return lax.dot_general(a, b, (contract, ((), ())), preferred_element_type=jnp.float32)


def parity_of_device():
    bits = lax.axis_index("grp") ^ lax.axis_index("row") ^ lax.axis_index("col")
    for shift in (8, 4, 2, 1):
        bits = bits ^ (bits >> shift)
    return bits & 1


def inverse_of(level_ref, parent_level, levels):
    found = jnp.int32(0)
    for level in range(levels):
        found = found + jnp.where(level_ref[level] == parent_level, level, 0)
    return found


def first_kernel(
    groups, columns, tile_hbm, cols_hbm, level_hbm, rate_hbm, spread_hbm, rows_hbm,
    averaged, keep, send, tile, spread, rows, places, rate,
    cols, sums, projected, level_index, sems,
):
    levels, tile_rows, tile_cols = tile.shape
    third_rows, third_cols = tile_rows // 3, tile_cols // 3
    group, _, col = (lax.axis_index(a) for a in AXES)
    is_parent = group == groups - 1
    slot = jnp.where(is_parent, (groups - 1) * columns + col, col * (groups - 1) + group)
    own_third = pl.ds(pl.multiple_of(group * third_cols, third_cols), third_cols)
    own_cols = pltpu.make_async_copy(
        cols_hbm.at[col, own_third], cols.at[pl.ds(0, third_cols)], sems.at[1]
    )
    all_cols = pltpu.make_async_copy(cols_hbm.at[col], cols, sems.at[1])
    copies = [
        pltpu.make_async_copy(tile_hbm, tile, sems.at[0]),
        pltpu.make_async_copy(level_hbm, level_index, sems.at[2]),
    ]
    later = [
        pltpu.make_async_copy(spread_hbm.at[slot], spread, sems.at[3]),
        pltpu.make_async_copy(rows_hbm, rows, sems.at[4]),
        pltpu.make_async_copy(rate_hbm, rate, sems.at[6]),
    ]
    for copy in copies:
        copy.start()
    pl.when(is_parent)(all_cols.start)
    pl.when(jnp.logical_not(is_parent))(own_cols.start)
    for copy in later:
        copy.start()
    lanes = sums.shape[-1]
    depth = 3 * lanes
    cell = lax.broadcasted_iota(jnp.int32, (depth, lanes), 0)
    block = 3 * lax.broadcasted_iota(jnp.int32, (depth, lanes), 1)
    pick = jnp.where((cell >= block) & (cell < block + 3), 1.0, 0.0).astype(jnp.bfloat16)
    for copy in copies:
        copy.wait()

    def project(blocks, table):
        left = lax.broadcasted_iota(jnp.int32, table.shape, 1) < BASIS
        zero = jnp.zeros_like(table)
        both = jnp.concatenate([jnp.where(left, table, zero), jnp.where(left, zero, table)], 0)
        pairs = [jnp.concatenate(blocks[k : k + 2], axis=1) for k in range(0, levels, 2)]
        values = dot(jnp.concatenate(pairs, axis=0), both)
        height = blocks[0].shape[0]
        for pair in range(levels // 2):
            projected[pair, pl.ds(0, height)] = values[pair * height : (pair + 1) * height]

    @pl.when(jnp.logical_not(is_parent))
    def _():
        flat = tile[...].reshape(levels * tile_rows, tile_cols)
        for part in range(third_cols // lanes):
            piece = dot(flat[:, part * depth : (part + 1) * depth], pick)
            sums[part] = piece.reshape(levels, tile_rows, lanes)
        blocks = []
        for parent_level in range(levels):
            level = inverse_of(level_index, parent_level, levels)
            totals = [
                sum(sums[part, level, pl.ds(a, third_rows, 3), :] for a in range(3))
                for part in range(third_cols // lanes)
            ]
            block = (jnp.concatenate(totals, axis=1) * (1.0 / 9.0)).astype(jnp.bfloat16)
            averaged[:, parent_level * third_cols : (parent_level + 1) * third_cols] = block
            blocks.append(block)
        projected[...] = jnp.zeros_like(projected)
        own_cols.wait()
        project(blocks, cols[pl.ds(0, third_cols), :])

    @pl.when(is_parent)
    def _():
        averaged[...] = jnp.zeros_like(averaged)
        all_cols.wait()
        project([tile[level] for level in range(levels)], cols[...])

    half = parity_of_device()
    keep[...] = projected[half]
    send[...] = projected[1 - half]
    for parent_level in range(levels):
        found = inverse_of(level_index, parent_level, levels)
        places[parent_level] = jnp.where(is_parent, parent_level, found)
    for copy in later:
        copy.wait()


def coeffs_kernel(full_rows, groups, offset, mine, partner, rows, out):
    tile_rows = mine.shape[0]
    group, row = lax.axis_index("grp"), lax.axis_index("row")
    shift = offset[0]
    cell = lax.broadcasted_iota(jnp.int32, (tile_rows, BASIS), 0)
    strip = lax.rem(row * tile_rows + cell - shift + full_rows, full_rows)
    strip_start = lax.rem(row * (tile_rows // 3) + shift, full_rows)

    def weights(is_parent):
        start = jnp.where(is_parent, row * tile_rows, strip_start)
        counted = jnp.where(is_parent, strip - full_rows // 3, tile_rows // 3 - 1 - cell) >= 0
        return jnp.where(counted, rows[pl.ds(start, tile_rows), :][:, :BASIS], 0.0).astype(
            jnp.bfloat16
        )

    table = jnp.concatenate([weights(group == groups - 1), weights((group ^ 1) == groups - 1)], 0)
    high, low = split(jnp.concatenate([mine[...], partner[...]], axis=0))
    out[...] = dot(table, high, ((0,), (0,))) + dot(table, low, ((0,), (0,)))


def select_kernel(
    full_rows, groups, exchanges, amplitude, offset, first, second, rows, driving, out, weights, target,
):
    tile_rows = out.shape[0]
    third_rows = tile_rows // 3
    row = lax.axis_index("row")
    is_parent = lax.axis_index("grp") == groups - 1
    shape = (tile_rows, first.shape[0] + second.shape[0])
    cell = lax.broadcasted_iota(jnp.int32, shape, 0)
    wanted = lax.rem(row * tile_rows + cell - offset[0] + full_rows, full_rows)
    place = lax.broadcasted_iota(jnp.int32, shape, 1)
    block = place // third_rows
    source = jnp.zeros_like(block)
    for step in range(exchanges):
        source = source + ((block >> step) & 1) * (1 << (exchanges - 1 - step))
    held = (row ^ source) * third_rows + place % third_rows
    pick = jnp.where(wanted == held, 1.0, 0.0).astype(jnp.bfloat16)
    strip = jnp.concatenate([first[...], second[...]], axis=0)
    out[...] = dot(pick, strip).astype(jnp.bfloat16)
    period = 3 * full_rows
    child_start = lax.rem(3 * offset[0] + row * tile_rows - 1 + period, period)
    own = pl.ds(pl.multiple_of(full_rows + (row + 1) * tile_rows, 8), tile_rows)
    high, low = split(
        jnp.where(
            is_parent, rows[own, :][:, :BASIS], rows[pl.ds(child_start, tile_rows), :][:, BASIS:]
        )
    )
    weights[...] = jnp.concatenate([high, low, high], axis=1)
    for pair in range(target.shape[0]):
        both = [driving[2 * pair], driving[2 * pair + 1]]
        target[pair] = amplitude * jnp.concatenate(both, axis=1)


def final_kernel(full_rows, groups, own_half, offset, places, rate, *refs):
    coeffs, spread, weights, target = refs[:4]
    group, row = lax.axis_index("grp"), lax.axis_index("row")
    is_parent = group == groups - 1
    half = parity_of_device()
    pair = half if own_half else 1 - half
    if own_half:
        tile, selected, block_0, block_1, block_2, result, later_base, left, base = refs[4:]
    else:
        earlier, base, out_hbm, left, result, sems = refs[4:]
    _, tile_rows, tile_cols = base.shape
    third_cols = tile_cols // 3
    copies = []

    def write(source, side, pair):
        place = out_hbm.at[places[2 * pair + side]]
        copies.append(pltpu.make_async_copy(source.at[side], place, sems.at[len(copies)]))
        copies[-1].start()

    if not own_half:
        write(earlier, 0, half)
        write(earlier, 1, half)
    high, low = split(target[pair] - coeffs[...])
    turned = dot(weights[...], jnp.concatenate([high, high, low], axis=0))
    is_left = lax.broadcasted_iota(jnp.int32, (tile_rows, 2 * BASIS), 1) < BASIS
    for side in range(2):
        high, low = split(turned * rate[2 * pair + side])
        low = pltpu.roll(low.astype(jnp.float32), BASIS, 1).astype(jnp.bfloat16)
        here = is_left if side == 0 else ~is_left
        span = pl.ds(side * tile_rows, tile_rows)
        left[span, : 2 * BASIS] = jnp.where(here, high, low)
        left[span, 2 * BASIS :] = jnp.where(here, high, jnp.zeros_like(high))
    high, low = spread[0], spread[1]
    increment = dot(left[...], jnp.concatenate([high, high, low, low], axis=0))

    if own_half:

        def feed(blocks):
            cell = lax.broadcasted_iota(jnp.int32, (tile_rows, third_cols), 0)
            strip = lax.rem(row * tile_rows + cell - offset[0] + full_rows, full_rows)
            covered = strip < full_rows // 3
            for goal, goal_pair in ((base, half), (later_base, 1 - half)):
                for side in range(2):
                    level = 2 * goal_pair + side
                    for third, block in enumerate(blocks):
                        span = slice(third * third_cols, (third + 1) * third_cols)
                        lanes = pl.ds(pl.multiple_of(level * third_cols, 128), third_cols)
                        arrived = block[:, lanes].astype(jnp.float32)
                        own = tile[level, :, span].astype(jnp.float32)
                        goal[side, :, span] = jnp.where(covered, arrived, own)

        even = half == 0
        pl.when(is_parent & even)(lambda: feed((block_0, block_1, selected)))
        pl.when(is_parent & jnp.logical_not(even))(lambda: feed((block_1, block_0, block_2)))

        @pl.when(jnp.logical_not(is_parent))
        def _():
            for goal, goal_pair in ((base, half), (later_base, 1 - half)):
                for side in range(2):
                    goal[side] = tile[places[2 * goal_pair + side]].astype(jnp.float32)

    for side in range(2):
        rows = increment[side * tile_rows : (side + 1) * tile_rows]
        result[side] = (base[side] + rows).astype(jnp.bfloat16)
        if not own_half:
            write(result, side, pair)
    for copy in copies:
        copy.wait()


def per_device(sizes, fields, offset, level_index, nudge_rate, driving):
    groups, row_count, col_count = sizes
    tile_in = fields[0]
    levels, tile_rows, tile_cols = tile_in.shape
    third_rows, third_cols = tile_rows // 3, tile_cols // 3
    full_rows, full_cols = row_count * tile_rows, col_count * tile_cols
    f32, bf16 = jnp.float32, jnp.bfloat16

    cols = basis_table(3 * np.arange(full_cols), full_cols)
    cols_twice = np.concatenate([cols, cols], 1).reshape(col_count, tile_cols, 2 * BASIS)
    cols_twice = cols_twice.astype(bf16)
    parent_rows = basis_table(3 * np.arange(full_rows), full_rows)
    rounded = parent_rows.astype(bf16).astype(np.float32)
    rounded = np.concatenate([rounded, rounded[:tile_rows]], 0)
    child_rows = basis_table(np.arange(3 * full_rows), full_rows)
    row_table = np.zeros((3 * full_rows + tile_rows, 2 * BASIS), np.float32)
    row_table[: 2 * full_rows + tile_rows, :BASIS] = np.concatenate([rounded, parent_rows], 0)
    row_table[:, BASIS:] = np.concatenate([child_rows, child_rows[:tile_rows]], 0)
    child_cols = basis_table((np.arange(3 * full_cols) - 1) % (3 * full_cols), full_cols)
    spread_rows = np.concatenate([child_cols, cols], 0).reshape(-1, tile_cols, BASIS)
    spread_rows = spread_rows.transpose(0, 2, 1)
    spread_table = np.stack(halves(spread_rows), 1)
    amplitude = math.sqrt(full_rows * full_cols) / BASIS

    def mask_of(group_bits, row_bits, col_bits):
        return (group_bits * row_count + row_bits) * col_count + col_bits

    def exchange(value, mask, odd_mask=None):
        masks = (mask, mask if odd_mask is None else odd_mask)
        count = groups * row_count * col_count
        pairs = [(i, i ^ masks[i.bit_count() % 2]) for i in range(count)]
        return lax.ppermute(value, AXES, pairs)

    flip = mask_of(1, 0, 0)
    across = [mask_of(1 << k, 0, 0) ^ flip for k in range(1, groups.bit_length() - 1)]
    across += [mask_of(0, 0, 1 << k) ^ flip for k in range(col_count.bit_length() - 1)]
    row_bits = [1 << k for k in reversed(range(row_count.bit_length() - 1))]
    along = [mask_of(0, bit, 0) ^ flip for bit in row_bits]
    along = along[::-1]
    rounds = across + along
    odd_rounds = across[:1] + along[:1] + across[1:] + along[1:]

    averaged, keep, send, tile, spread, rows, places, rate = pl.pallas_call(
        functools.partial(first_kernel, groups, col_count),
        out_shape=(
            pltpu.VMEM((third_rows, levels * third_cols), bf16),
            pltpu.VMEM((tile_rows, 2 * BASIS), f32),
            pltpu.VMEM((tile_rows, 2 * BASIS), f32),
            pltpu.VMEM(tile_in.shape, bf16),
            pltpu.VMEM((2, BASIS, tile_cols), bf16),
            pltpu.VMEM(row_table.shape, f32),
            pltpu.SMEM((levels,), jnp.int32),
            pltpu.SMEM((levels,), f32),
        ),
        in_specs=[ANY] * 6,
        out_specs=(VMEM,) * 6 + (SMEM, SMEM),
        scratch_shapes=[
            pltpu.VMEM((tile_cols, 2 * BASIS), bf16),
            pltpu.VMEM((third_cols // 128, levels, tile_rows, 128), f32),
            pltpu.VMEM((levels // 2, tile_rows, 2 * BASIS), f32),
            pltpu.SMEM((levels,), jnp.int32),
            pltpu.SemaphoreType.DMA((7,)),
        ],
        name="first",
    )(
        tile_in, jnp.asarray(cols_twice), in_hbm(level_index), in_hbm(nudge_rate),
        jnp.asarray(spread_table), jnp.asarray(row_table),
    )

    partner = exchange(send, flip)
    mine = pl.pallas_call(
        functools.partial(coeffs_kernel, full_rows, groups),
        out_shape=pltpu.VMEM((BASIS, 2 * BASIS), f32),
        in_specs=[SMEM, VMEM, VMEM, VMEM],
        out_specs=VMEM,
        name="coeffs",
    )(offset, in_vmem(keep), in_vmem(partner), in_vmem(rows))
    for masks in zip(rounds, odd_rounds):
        mine = mine + exchange(mine, masks[0], masks[1])
    other = exchange(mine, flip)

    pair = exchange(averaged, flip)
    strips = [jnp.where(parity_of_device() == lax.axis_index("grp") % 2, averaged, pair)]
    for step, bit in enumerate(row_bits):
        held = strips[0] if step == 0 else jnp.concatenate(strips, 0)
        strips = [held, exchange(held, mask_of(0, bit, 0) ^ flip)]
    selected, weights, target = pl.pallas_call(
        functools.partial(select_kernel, full_rows, groups, len(row_bits), amplitude),
        out_shape=(
            pltpu.VMEM((tile_rows, levels * third_cols), bf16),
            pltpu.VMEM((tile_rows, 3 * BASIS), bf16),
            pltpu.VMEM((levels // 2, BASIS, 2 * BASIS), f32),
        ),
        in_specs=[SMEM] + [VMEM] * 4,
        out_specs=(VMEM,) * 3,
        name="select",
    )(offset, *(in_vmem(value) for value in (*strips, rows, driving)))
    block_0 = exchange(selected, mask_of(3, 0, 0))
    block_2 = exchange(selected, mask_of(1, 0, 0))
    block_1 = exchange(block_0, mask_of(1, 0, 0))

    def finish(name, coeffs, values, out_shape, out_spec, scratch):
        values = (coeffs, spread, weights, target, *values)
        return pl.pallas_call(
            functools.partial(final_kernel, full_rows, groups, name == "final_own"),
            out_shape=out_shape,
            in_specs=[SMEM] * 3 + [VMEM] * len(values),
            out_specs=out_spec,
            scratch_shapes=[pltpu.VMEM((2 * tile_rows, 4 * BASIS), bf16), *scratch],
        )(offset, places, rate, *(in_vmem(value) for value in values))

    two_levels = (2, tile_rows, tile_cols)
    earlier = finish(
        "final_own", mine, (tile, selected, block_0, block_1, block_2),
        (pltpu.VMEM(two_levels, bf16), pltpu.VMEM(two_levels, f32)), (VMEM, VMEM),
        [pltpu.VMEM(two_levels, f32)],
    )
    result = finish(
        "final_other", other, earlier, jax.ShapeDtypeStruct(tile_in.shape, bf16), ANY,
        [pltpu.VMEM(two_levels, bf16), pltpu.SemaphoreType.DMA((4,))],
    )
    return result[None]


def solution(mesh):
    placed = (P("grp", None, "row", "col"), P(), P(), P(), P())
    sizes = tuple(mesh.shape[axis] for axis in AXES)
    return jax.shard_map(
        functools.partial(per_device, sizes),
        mesh=mesh,
        in_specs=placed,
        out_specs=P("grp", None, "row", "col"),
        check_vma=False,
    )
```

```python
import functools
import math

import jax
import jax.numpy as jnp
import numpy as np
from jax import lax
from jax.experimental import pallas as pl
from jax.experimental.pallas import tpu as pltpu
from jax.sharding import PartitionSpec as P

MAX_WAVE = 32
BASIS = 2 * MAX_WAVE
AXES = ("grp", "row", "col")
VMEM = pl.BlockSpec(memory_space=pltpu.VMEM)
SMEM = pl.BlockSpec(memory_space=pltpu.SMEM)
ANY = pl.BlockSpec(memory_space=pl.ANY)


def in_vmem(value):
    return pltpu.with_memory_space_constraint(value, pltpu.VMEM)


def in_hbm(value):
    return pltpu.with_memory_space_constraint(value, pltpu.HBM)


def basis_table(positions, cell_count):
    period = 3 * cell_count
    orders = np.arange(1, MAX_WAVE + 1)
    angles = (np.asarray(positions)[:, None] * orders % period) * (2.0 * math.pi / period)
    scale = math.sqrt(2.0 / cell_count)
    constant = np.full((len(positions), 1), 1.0 / math.sqrt(cell_count))
    table = np.concatenate([constant, scale * np.cos(angles), scale * np.sin(angles[:, :-1])], 1)
    return table.astype(np.float32)


def halves(table):
    high = table.astype(jnp.bfloat16)
    return high, (table - high.astype(np.float32)).astype(jnp.bfloat16)


def split(value):
    high = value.astype(jnp.bfloat16)
    return high, (value - high.astype(jnp.float32)).astype(jnp.bfloat16)


def dot(a, b, contract=((1,), (0,))):
    return lax.dot_general(a, b, (contract, ((), ())), preferred_element_type=jnp.float32)


def parity_of_device():
    bits = lax.axis_index("grp") ^ lax.axis_index("row") ^ lax.axis_index("col")
    for shift in (8, 4, 2, 1):
        bits = bits ^ (bits >> shift)
    return bits & 1


def inverse_of(level_ref, parent_level, levels):
    found = jnp.int32(0)
    for level in range(levels):
        found = found + jnp.where(level_ref[level] == parent_level, level, 0)
    return found


def first_kernel(
    groups, columns, tile_hbm, cols_hbm, level_hbm, rate_hbm, spread_hbm, rows_hbm,
    averaged, keep, send, tile, spread, rows, places, rate,
    cols, sums, projected, level_index, sems,
):
    levels, tile_rows, tile_cols = tile.shape
    third_rows, third_cols = tile_rows // 3, tile_cols // 3
    group, _, col = (lax.axis_index(a) for a in AXES)
    is_parent = group == groups - 1
    slot = jnp.where(is_parent, (groups - 1) * columns + col, col * (groups - 1) + group)
    own_third = pl.ds(pl.multiple_of(group * third_cols, third_cols), third_cols)
    own_cols = pltpu.make_async_copy(
        cols_hbm.at[col, own_third], cols.at[pl.ds(0, third_cols)], sems.at[1]
    )
    all_cols = pltpu.make_async_copy(cols_hbm.at[col], cols, sems.at[1])
    copies = [
        pltpu.make_async_copy(tile_hbm, tile, sems.at[0]),
        pltpu.make_async_copy(level_hbm, level_index, sems.at[2]),
    ]
    later = [
        pltpu.make_async_copy(spread_hbm.at[slot], spread, sems.at[3]),
        pltpu.make_async_copy(rows_hbm, rows, sems.at[4]),
        pltpu.make_async_copy(rate_hbm, rate, sems.at[6]),
    ]
    for copy in copies:
        copy.start()
    pl.when(is_parent)(all_cols.start)
    pl.when(jnp.logical_not(is_parent))(own_cols.start)
    for copy in later:
        copy.start()
    lanes = sums.shape[-1]
    depth = 3 * lanes
    cell = lax.broadcasted_iota(jnp.int32, (depth, lanes), 0)
    block = 3 * lax.broadcasted_iota(jnp.int32, (depth, lanes), 1)
    pick = jnp.where((cell >= block) & (cell < block + 3), 1.0, 0.0).astype(jnp.bfloat16)
    for copy in copies:
        copy.wait()

    def project(blocks, table):
        left = lax.broadcasted_iota(jnp.int32, table.shape, 1) < BASIS
        zero = jnp.zeros_like(table)
        both = jnp.concatenate([jnp.where(left, table, zero), jnp.where(left, zero, table)], 0)
        pairs = [jnp.concatenate(blocks[k : k + 2], axis=1) for k in range(0, levels, 2)]
        values = dot(jnp.concatenate(pairs, axis=0), both)
        height = blocks[0].shape[0]
        for pair in range(levels // 2):
            projected[pair, pl.ds(0, height)] = values[pair * height : (pair + 1) * height]

    @pl.when(jnp.logical_not(is_parent))
    def _():
        flat = tile[...].reshape(levels * tile_rows, tile_cols)
        for part in range(third_cols // lanes):
            piece = dot(flat[:, part * depth : (part + 1) * depth], pick)
            sums[part] = piece.reshape(levels, tile_rows, lanes)
        blocks = []
        for parent_level in range(levels):
            level = inverse_of(level_index, parent_level, levels)
            totals = [
                sum(sums[part, level, pl.ds(a, third_rows, 3), :] for a in range(3))
                for part in range(third_cols // lanes)
            ]
            block = (jnp.concatenate(totals, axis=1) * (1.0 / 9.0)).astype(jnp.bfloat16)
            averaged[:, parent_level * third_cols : (parent_level + 1) * third_cols] = block
            blocks.append(block)
        projected[...] = jnp.zeros_like(projected)
        own_cols.wait()
        project(blocks, cols[pl.ds(0, third_cols), :])

    @pl.when(is_parent)
    def _():
        averaged[...] = jnp.zeros_like(averaged)
        all_cols.wait()
        project([tile[level] for level in range(levels)], cols[...])

    half = parity_of_device()
    keep[...] = projected[half]
    send[...] = projected[1 - half]
    for parent_level in range(levels):
        found = inverse_of(level_index, parent_level, levels)
        places[parent_level] = jnp.where(is_parent, parent_level, found)
    for copy in later:
        copy.wait()


def coeffs_kernel(full_rows, groups, offset, mine, partner, rows, out):
    tile_rows = mine.shape[0]
    group, row = lax.axis_index("grp"), lax.axis_index("row")
    shift = offset[0]
    cell = lax.broadcasted_iota(jnp.int32, (tile_rows, BASIS), 0)
    strip = lax.rem(row * tile_rows + cell - shift + full_rows, full_rows)
    strip_start = lax.rem(row * (tile_rows // 3) + shift, full_rows)

    def weights(is_parent):
        start = jnp.where(is_parent, row * tile_rows, strip_start)
        counted = jnp.where(is_parent, strip - full_rows // 3, tile_rows // 3 - 1 - cell) >= 0
        return jnp.where(counted, rows[pl.ds(start, tile_rows), :][:, :BASIS], 0.0).astype(
            jnp.bfloat16
        )

    table = jnp.concatenate([weights(group == groups - 1), weights((group ^ 1) == groups - 1)], 0)
    high, low = split(jnp.concatenate([mine[...], partner[...]], axis=0))
    out[...] = dot(
        jnp.concatenate([table, table], 0), jnp.concatenate([high, low], 0), ((0,), (0,))
    )


def select_kernel(
    full_rows, groups, exchanges, amplitude, offset, first, second, rows, driving, out, weights, target,
):
    tile_rows = out.shape[0]
    third_rows = tile_rows // 3
    row = lax.axis_index("row")
    is_parent = lax.axis_index("grp") == groups - 1
    shape = (tile_rows, first.shape[0] + second.shape[0])
    cell = lax.broadcasted_iota(jnp.int32, shape, 0)
    wanted = lax.rem(row * tile_rows + cell - offset[0] + full_rows, full_rows)
    place = lax.broadcasted_iota(jnp.int32, shape, 1)
    block = place // third_rows
    source = jnp.zeros_like(block)
    for step in range(exchanges):
        source = source + ((block >> step) & 1) * (1 << (exchanges - 1 - step))
    held = (row ^ source) * third_rows + place % third_rows
    pick = jnp.where(wanted == held, 1.0, 0.0).astype(jnp.bfloat16)
    strip = jnp.concatenate([first[...], second[...]], axis=0)
    out[...] = dot(pick, strip).astype(jnp.bfloat16)
    period = 3 * full_rows
    child_start = lax.rem(3 * offset[0] + row * tile_rows - 1 + period, period)
    own = pl.ds(pl.multiple_of(full_rows + (row + 1) * tile_rows, 8), tile_rows)
    high, low = split(
        jnp.where(
            is_parent, rows[own, :][:, :BASIS], rows[pl.ds(child_start, tile_rows), :][:, BASIS:]
        )
    )
    weights[...] = jnp.concatenate([high, low, high], axis=1)
    for pair in range(target.shape[0]):
        both = [driving[2 * pair], driving[2 * pair + 1]]
        target[pair] = amplitude * jnp.concatenate(both, axis=1)


def final_kernel(full_rows, groups, own_half, offset, places, rate, *refs):
    coeffs, spread, weights, target = refs[:4]
    group, row = lax.axis_index("grp"), lax.axis_index("row")
    is_parent = group == groups - 1
    half = parity_of_device()
    pair = half if own_half else 1 - half
    if own_half:
        tile, selected, block_0, block_1, block_2, result, later_base, left, base = refs[4:]
    else:
        earlier, base, out_hbm, left, result, sems = refs[4:]
    _, tile_rows, tile_cols = base.shape
    third_cols = tile_cols // 3
    copies = []

    def write(source, side, pair):
        place = out_hbm.at[places[2 * pair + side]]
        copies.append(pltpu.make_async_copy(source.at[side], place, sems.at[len(copies)]))
        copies[-1].start()

    if not own_half:
        write(earlier, 0, half)
        write(earlier, 1, half)
    high, low = split(target[pair] - coeffs[...])
    turned = dot(weights[...], jnp.concatenate([high, high, low], axis=0))
    is_left = lax.broadcasted_iota(jnp.int32, (tile_rows, 2 * BASIS), 1) < BASIS
    for side in range(2):
        high, low = split(turned * rate[2 * pair + side])
        low = pltpu.roll(low.astype(jnp.float32), BASIS, 1).astype(jnp.bfloat16)
        here = is_left if side == 0 else ~is_left
        span = pl.ds(side * tile_rows, tile_rows)
        left[span, : 2 * BASIS] = jnp.where(here, high, low)
        left[span, 2 * BASIS :] = jnp.where(here, high, jnp.zeros_like(high))
    high, low = spread[0], spread[1]
    increment = dot(left[...], jnp.concatenate([high, high, low, low], axis=0))

    if own_half:

        def feed(blocks):
            cell = lax.broadcasted_iota(jnp.int32, (tile_rows, third_cols), 0)
            strip = lax.rem(row * tile_rows + cell - offset[0] + full_rows, full_rows)
            covered = strip < full_rows // 3
            for goal, goal_pair in ((base, half), (later_base, 1 - half)):
                for side in range(2):
                    level = 2 * goal_pair + side
                    for third, block in enumerate(blocks):
                        span = slice(third * third_cols, (third + 1) * third_cols)
                        lanes = pl.ds(pl.multiple_of(level * third_cols, 128), third_cols)
                        arrived = block[:, lanes].astype(jnp.float32)
                        own = tile[level, :, span].astype(jnp.float32)
                        goal[side, :, span] = jnp.where(covered, arrived, own)

        even = half == 0
        pl.when(is_parent & even)(lambda: feed((block_0, block_1, selected)))
        pl.when(is_parent & jnp.logical_not(even))(lambda: feed((block_1, block_0, block_2)))

        @pl.when(jnp.logical_not(is_parent))
        def _():
            for goal, goal_pair in ((base, half), (later_base, 1 - half)):
                for side in range(2):
                    goal[side] = tile[places[2 * goal_pair + side]].astype(jnp.float32)

    for side in range(2):
        rows = increment[side * tile_rows : (side + 1) * tile_rows]
        result[side] = (base[side] + rows).astype(jnp.bfloat16)
        if not own_half:
            write(result, side, pair)
    for copy in copies:
        copy.wait()


def per_device(sizes, fields, offset, level_index, nudge_rate, driving):
    groups, row_count, col_count = sizes
    tile_in = fields[0]
    levels, tile_rows, tile_cols = tile_in.shape
    third_rows, third_cols = tile_rows // 3, tile_cols // 3
    full_rows, full_cols = row_count * tile_rows, col_count * tile_cols
    f32, bf16 = jnp.float32, jnp.bfloat16

    cols = basis_table(3 * np.arange(full_cols), full_cols)
    cols_twice = np.concatenate([cols, cols], 1).reshape(col_count, tile_cols, 2 * BASIS)
    cols_twice = cols_twice.astype(bf16)
    parent_rows = basis_table(3 * np.arange(full_rows), full_rows)
    rounded = parent_rows.astype(bf16).astype(np.float32)
    rounded = np.concatenate([rounded, rounded[:tile_rows]], 0)
    child_rows = basis_table(np.arange(3 * full_rows), full_rows)
    row_table = np.zeros((3 * full_rows + tile_rows, 2 * BASIS), np.float32)
    row_table[: 2 * full_rows + tile_rows, :BASIS] = np.concatenate([rounded, parent_rows], 0)
    row_table[:, BASIS:] = np.concatenate([child_rows, child_rows[:tile_rows]], 0)
    child_cols = basis_table((np.arange(3 * full_cols) - 1) % (3 * full_cols), full_cols)
    spread_rows = np.concatenate([child_cols, cols], 0).reshape(-1, tile_cols, BASIS)
    spread_rows = spread_rows.transpose(0, 2, 1)
    spread_table = np.stack(halves(spread_rows), 1)
    amplitude = math.sqrt(full_rows * full_cols) / BASIS

    def mask_of(group_bits, row_bits, col_bits):
        return (group_bits * row_count + row_bits) * col_count + col_bits

    def exchange(value, mask, odd_mask=None):
        masks = (mask, mask if odd_mask is None else odd_mask)
        count = groups * row_count * col_count
        pairs = [(i, i ^ masks[i.bit_count() % 2]) for i in range(count)]
        return lax.ppermute(value, AXES, pairs)

    flip = mask_of(1, 0, 0)
    across = [mask_of(1 << k, 0, 0) ^ flip for k in range(1, groups.bit_length() - 1)]
    across += [mask_of(0, 0, 1 << k) ^ flip for k in range(col_count.bit_length() - 1)]
    row_bits = [1 << k for k in reversed(range(row_count.bit_length() - 1))]
    along = [mask_of(0, bit, 0) ^ flip for bit in row_bits]
    along = along[::-1]
    rounds = across + along
    odd_rounds = across[:1] + along[:1] + across[1:] + along[1:]

    averaged, keep, send, tile, spread, rows, places, rate = pl.pallas_call(
        functools.partial(first_kernel, groups, col_count),
        out_shape=(
            pltpu.VMEM((third_rows, levels * third_cols), bf16),
            pltpu.VMEM((tile_rows, 2 * BASIS), f32),
            pltpu.VMEM((tile_rows, 2 * BASIS), f32),
            pltpu.VMEM(tile_in.shape, bf16),
            pltpu.VMEM((2, BASIS, tile_cols), bf16),
            pltpu.VMEM(row_table.shape, f32),
            pltpu.SMEM((levels,), jnp.int32),
            pltpu.SMEM((levels,), f32),
        ),
        in_specs=[ANY] * 6,
        out_specs=(VMEM,) * 6 + (SMEM, SMEM),
        scratch_shapes=[
            pltpu.VMEM((tile_cols, 2 * BASIS), bf16),
            pltpu.VMEM((third_cols // 128, levels, tile_rows, 128), f32),
            pltpu.VMEM((levels // 2, tile_rows, 2 * BASIS), f32),
            pltpu.SMEM((levels,), jnp.int32),
            pltpu.SemaphoreType.DMA((7,)),
        ],
        name="first",
    )(
        tile_in, jnp.asarray(cols_twice), in_hbm(level_index), in_hbm(nudge_rate),
        jnp.asarray(spread_table), jnp.asarray(row_table),
    )

    partner = exchange(send, flip)
    mine = pl.pallas_call(
        functools.partial(coeffs_kernel, full_rows, groups),
        out_shape=pltpu.VMEM((BASIS, 2 * BASIS), f32),
        in_specs=[SMEM, VMEM, VMEM, VMEM],
        out_specs=VMEM,
        name="coeffs",
    )(offset, in_vmem(keep), in_vmem(partner), in_vmem(rows))
    for masks in zip(rounds, odd_rounds):
        mine = mine + exchange(mine, masks[1], masks[0])
    other = exchange(mine, flip)

    pair = exchange(averaged, flip)
    strips = [jnp.where(parity_of_device() == lax.axis_index("grp") % 2, averaged, pair)]
    for step, bit in enumerate(row_bits):
        held = strips[0] if step == 0 else jnp.concatenate(strips, 0)
        strips = [held, exchange(held, mask_of(0, bit, 0) ^ flip)]
    selected, weights, target = pl.pallas_call(
        functools.partial(select_kernel, full_rows, groups, len(row_bits), amplitude),
        out_shape=(
            pltpu.VMEM((tile_rows, levels * third_cols), bf16),
            pltpu.VMEM((tile_rows, 3 * BASIS), bf16),
            pltpu.VMEM((levels // 2, BASIS, 2 * BASIS), f32),
        ),
        in_specs=[SMEM] + [VMEM] * 4,
        out_specs=(VMEM,) * 3,
        name="select",
    )(offset, *(in_vmem(value) for value in (*strips, rows, driving)))
    block_0 = exchange(selected, mask_of(3, 0, 0))
    block_2 = exchange(selected, mask_of(1, 0, 0))
    block_1 = exchange(block_0, mask_of(1, 0, 0))

    def finish(name, coeffs, values, out_shape, out_spec, scratch):
        values = (coeffs, spread, weights, target, *values)
        return pl.pallas_call(
            functools.partial(final_kernel, full_rows, groups, name == "final_own"),
            out_shape=out_shape,
            in_specs=[SMEM] * 3 + [VMEM] * len(values),
            out_specs=out_spec,
            scratch_shapes=[pltpu.VMEM((2 * tile_rows, 4 * BASIS), bf16), *scratch],
        )(offset, places, rate, *(in_vmem(value) for value in values))

    two_levels = (2, tile_rows, tile_cols)
    earlier = finish(
        "final_own", mine, (tile, selected, block_0, block_1, block_2),
        (pltpu.VMEM(two_levels, bf16), pltpu.VMEM(two_levels, f32)), (VMEM, VMEM),
        [pltpu.VMEM(two_levels, f32)],
    )
    result = finish(
        "final_other", other, earlier, jax.ShapeDtypeStruct(tile_in.shape, bf16), ANY,
        [pltpu.VMEM(two_levels, bf16), pltpu.SemaphoreType.DMA((4,))],
    )
    return result[None]


def solution(mesh):
    placed = (P("grp", None, "row", "col"), P(), P(), P(), P())
    sizes = tuple(mesh.shape[axis] for axis in AXES)
    return jax.shard_map(
        functools.partial(per_device, sizes),
        mesh=mesh,
        in_specs=placed,
        out_specs=P("grp", None, "row", "col"),
        check_vma=False,
    )
```

```python
import functools
import math

import jax
import jax.numpy as jnp
import numpy as np
from jax import lax
from jax.experimental import pallas as pl
from jax.experimental.pallas import tpu as pltpu
from jax.sharding import PartitionSpec as P

MAX_WAVE = 32
BASIS = 2 * MAX_WAVE
AXES = ("grp", "row", "col")
VMEM = pl.BlockSpec(memory_space=pltpu.VMEM)
SMEM = pl.BlockSpec(memory_space=pltpu.SMEM)
ANY = pl.BlockSpec(memory_space=pl.ANY)


def in_vmem(value):
    return pltpu.with_memory_space_constraint(value, pltpu.VMEM)


def in_hbm(value):
    return pltpu.with_memory_space_constraint(value, pltpu.HBM)


def basis_table(positions, cell_count):
    period = 3 * cell_count
    orders = np.arange(1, MAX_WAVE + 1)
    angles = (np.asarray(positions)[:, None] * orders % period) * (2.0 * math.pi / period)
    scale = math.sqrt(2.0 / cell_count)
    constant = np.full((len(positions), 1), 1.0 / math.sqrt(cell_count))
    table = np.concatenate([constant, scale * np.cos(angles), scale * np.sin(angles[:, :-1])], 1)
    return table.astype(np.float32)


def halves(table):
    high = table.astype(jnp.bfloat16)
    return high, (table - high.astype(np.float32)).astype(jnp.bfloat16)


def split(value):
    high = value.astype(jnp.bfloat16)
    return high, (value - high.astype(jnp.float32)).astype(jnp.bfloat16)


def dot(a, b, contract=((1,), (0,))):
    return lax.dot_general(a, b, (contract, ((), ())), preferred_element_type=jnp.float32)


def parity_of_device():
    bits = lax.axis_index("grp") ^ lax.axis_index("row") ^ lax.axis_index("col")
    for shift in (8, 4, 2, 1):
        bits = bits ^ (bits >> shift)
    return bits & 1


def inverse_of(level_ref, parent_level, levels):
    found = jnp.int32(0)
    for level in range(levels):
        found = found + jnp.where(level_ref[level] == parent_level, level, 0)
    return found


def first_kernel(
    groups, columns, tile_hbm, cols_hbm, level_hbm, rate_hbm, spread_hbm, rows_hbm,
    averaged, keep, send, tile, spread, rows, places, rate,
    cols, sums, projected, level_index, sems,
):
    levels, tile_rows, tile_cols = tile.shape
    third_rows, third_cols = tile_rows // 3, tile_cols // 3
    group, _, col = (lax.axis_index(a) for a in AXES)
    is_parent = group == groups - 1
    slot = jnp.where(is_parent, (groups - 1) * columns + col, col * (groups - 1) + group)
    own_third = pl.ds(pl.multiple_of(group * third_cols, third_cols), third_cols)
    own_cols = pltpu.make_async_copy(
        cols_hbm.at[col, own_third], cols.at[pl.ds(0, third_cols)], sems.at[1]
    )
    all_cols = pltpu.make_async_copy(cols_hbm.at[col], cols, sems.at[1])
    copies = [
        pltpu.make_async_copy(tile_hbm, tile, sems.at[0]),
        pltpu.make_async_copy(level_hbm, level_index, sems.at[2]),
    ]
    later = [
        pltpu.make_async_copy(spread_hbm.at[slot], spread, sems.at[3]),
        pltpu.make_async_copy(rows_hbm, rows, sems.at[4]),
        pltpu.make_async_copy(rate_hbm, rate, sems.at[6]),
    ]
    for copy in copies:
        copy.start()
    pl.when(is_parent)(all_cols.start)
    pl.when(jnp.logical_not(is_parent))(own_cols.start)
    for copy in later:
        copy.start()
    lanes = sums.shape[-1]
    depth = 3 * lanes
    cell = lax.broadcasted_iota(jnp.int32, (depth, lanes), 0)
    block = 3 * lax.broadcasted_iota(jnp.int32, (depth, lanes), 1)
    pick = jnp.where((cell >= block) & (cell < block + 3), 1.0, 0.0).astype(jnp.bfloat16)
    for copy in copies:
        copy.wait()

    def project(blocks, table):
        left = lax.broadcasted_iota(jnp.int32, table.shape, 1) < BASIS
        zero = jnp.zeros_like(table)
        both = jnp.concatenate([jnp.where(left, table, zero), jnp.where(left, zero, table)], 0)
        pairs = [jnp.concatenate(blocks[k : k + 2], axis=1) for k in range(0, levels, 2)]
        values = dot(jnp.concatenate(pairs, axis=0), both)
        height = blocks[0].shape[0]
        for pair in range(levels // 2):
            projected[pair, pl.ds(0, height)] = values[pair * height : (pair + 1) * height]

    @pl.when(jnp.logical_not(is_parent))
    def _():
        flat = tile[...].reshape(levels * tile_rows, tile_cols)
        for part in range(third_cols // lanes):
            piece = dot(flat[:, part * depth : (part + 1) * depth], pick)
            sums[part] = piece.reshape(levels, tile_rows, lanes)
        blocks = []
        for parent_level in range(levels):
            level = inverse_of(level_index, parent_level, levels)
            totals = [
                sum(sums[part, level, pl.ds(a, third_rows, 3), :] for a in range(3))
                for part in range(third_cols // lanes)
            ]
            block = (jnp.concatenate(totals, axis=1) * (1.0 / 9.0)).astype(jnp.bfloat16)
            averaged[:, parent_level * third_cols : (parent_level + 1) * third_cols] = block
            blocks.append(block)
        projected[...] = jnp.zeros_like(projected)
        own_cols.wait()
        project(blocks, cols[pl.ds(0, third_cols), :])

    @pl.when(is_parent)
    def _():
        averaged[...] = jnp.zeros_like(averaged)
        all_cols.wait()
        project([tile[level] for level in range(levels)], cols[...])

    half = parity_of_device()
    keep[...] = projected[half]
    send[...] = projected[1 - half]
    for parent_level in range(levels):
        found = inverse_of(level_index, parent_level, levels)
        places[parent_level] = jnp.where(is_parent, parent_level, found)
    for copy in later:
        copy.wait()


def coeffs_kernel(full_rows, groups, offset, mine, partner, rows, out):
    tile_rows = mine.shape[0]
    group, row = lax.axis_index("grp"), lax.axis_index("row")
    shift = offset[0]
    cell = lax.broadcasted_iota(jnp.int32, (tile_rows, BASIS), 0)
    strip = lax.rem(row * tile_rows + cell - shift + full_rows, full_rows)
    strip_start = lax.rem(row * (tile_rows // 3) + shift, full_rows)

    def weights(is_parent):
        start = jnp.where(is_parent, row * tile_rows, strip_start)
        counted = jnp.where(is_parent, strip - full_rows // 3, tile_rows // 3 - 1 - cell) >= 0
        return jnp.where(counted, rows[pl.ds(start, tile_rows), :][:, :BASIS], 0.0).astype(
            jnp.bfloat16
        )

    table = jnp.concatenate([weights(group == groups - 1), weights((group ^ 1) == groups - 1)], 0)
    high, low = split(jnp.concatenate([mine[...], partner[...]], axis=0))
    out[...] = dot(
        jnp.concatenate([table, table], 0), jnp.concatenate([high, low], 0), ((0,), (0,))
    )


def select_kernel(
    full_rows, groups, exchanges, amplitude, offset, first, second, rows, driving, out, weights, target,
):
    tile_rows = out.shape[0]
    third_rows = tile_rows // 3
    row = lax.axis_index("row")
    is_parent = lax.axis_index("grp") == groups - 1
    shape = (tile_rows, first.shape[0] + second.shape[0])
    cell = lax.broadcasted_iota(jnp.int32, shape, 0)
    wanted = lax.rem(row * tile_rows + cell - offset[0] + full_rows, full_rows)
    place = lax.broadcasted_iota(jnp.int32, shape, 1)
    block = place // third_rows
    source = jnp.zeros_like(block)
    for step in range(exchanges):
        source = source + ((block >> step) & 1) * (1 << (exchanges - 1 - step))
    held = (row ^ source) * third_rows + place % third_rows
    pick = jnp.where(wanted == held, 1.0, 0.0).astype(jnp.bfloat16)
    strip = jnp.concatenate([first[...], second[...]], axis=0)
    out[...] = dot(pick, strip).astype(jnp.bfloat16)
    period = 3 * full_rows
    child_start = lax.rem(3 * offset[0] + row * tile_rows - 1 + period, period)
    own = pl.ds(pl.multiple_of(full_rows + (row + 1) * tile_rows, 8), tile_rows)
    high, low = split(
        jnp.where(
            is_parent, rows[own, :][:, :BASIS], rows[pl.ds(child_start, tile_rows), :][:, BASIS:]
        )
    )
    weights[...] = jnp.concatenate([high, low, high], axis=1)
    for pair in range(target.shape[0]):
        both = [driving[2 * pair], driving[2 * pair + 1]]
        target[pair] = amplitude * jnp.concatenate(both, axis=1)


def final_kernel(full_rows, groups, own_half, offset, places, rate, *refs):
    coeffs, spread, weights, target = refs[:4]
    group, row = lax.axis_index("grp"), lax.axis_index("row")
    is_parent = group == groups - 1
    half = parity_of_device()
    pair = half if own_half else 1 - half
    if own_half:
        tile, selected, block_0, block_1, block_2, result, later_base, left, base = refs[4:]
    else:
        earlier, base, out_hbm, left, result, sems = refs[4:]
    _, tile_rows, tile_cols = base.shape
    third_cols = tile_cols // 3
    copies = []

    def write(source, side, pair):
        place = out_hbm.at[places[2 * pair + side]]
        copies.append(pltpu.make_async_copy(source.at[side], place, sems.at[len(copies)]))
        copies[-1].start()

    if not own_half:
        write(earlier, 0, half)
        write(earlier, 1, half)
    high, low = split(target[pair] - coeffs[...])
    turned = dot(weights[...], jnp.concatenate([high, high, low], axis=0))
    is_left = lax.broadcasted_iota(jnp.int32, (tile_rows, 2 * BASIS), 1) < BASIS
    for side in range(2):
        high, low = split(turned * rate[2 * pair + side])
        here = is_left if side == 0 else ~is_left
        zero = jnp.zeros_like(high)
        high, low = jnp.where(here, high, zero), jnp.where(here, low, zero)
        span = pl.ds(side * tile_rows, tile_rows)
        left[span, :] = jnp.concatenate([high, low, high], axis=1)
    high, low = spread[0], spread[1]
    increment = dot(left[...], jnp.concatenate([high, high, high, high, low, low], axis=0))

    if own_half:

        def feed(blocks):
            cell = lax.broadcasted_iota(jnp.int32, (tile_rows, third_cols), 0)
            strip = lax.rem(row * tile_rows + cell - offset[0] + full_rows, full_rows)
            covered = strip < full_rows // 3
            for goal, goal_pair in ((base, half), (later_base, 1 - half)):
                for side in range(2):
                    level = 2 * goal_pair + side
                    for third, block in enumerate(blocks):
                        span = slice(third * third_cols, (third + 1) * third_cols)
                        lanes = pl.ds(pl.multiple_of(level * third_cols, 128), third_cols)
                        arrived = block[:, lanes].astype(jnp.float32)
                        own = tile[level, :, span].astype(jnp.float32)
                        goal[side, :, span] = jnp.where(covered, arrived, own)

        even = half == 0
        pl.when(is_parent & even)(lambda: feed((block_0, block_1, selected)))
        pl.when(is_parent & jnp.logical_not(even))(lambda: feed((block_1, block_0, block_2)))

        @pl.when(jnp.logical_not(is_parent))
        def _():
            for goal, goal_pair in ((base, half), (later_base, 1 - half)):
                for side in range(2):
                    goal[side] = tile[places[2 * goal_pair + side]].astype(jnp.float32)

    for side in range(2):
        rows = increment[side * tile_rows : (side + 1) * tile_rows]
        result[side] = (base[side] + rows).astype(jnp.bfloat16)
        if not own_half:
            write(result, side, pair)
    for copy in copies:
        copy.wait()


def per_device(sizes, fields, offset, level_index, nudge_rate, driving):
    groups, row_count, col_count = sizes
    tile_in = fields[0]
    levels, tile_rows, tile_cols = tile_in.shape
    third_rows, third_cols = tile_rows // 3, tile_cols // 3
    full_rows, full_cols = row_count * tile_rows, col_count * tile_cols
    f32, bf16 = jnp.float32, jnp.bfloat16

    cols = basis_table(3 * np.arange(full_cols), full_cols)
    cols_twice = np.concatenate([cols, cols], 1).reshape(col_count, tile_cols, 2 * BASIS)
    cols_twice = cols_twice.astype(bf16)
    parent_rows = basis_table(3 * np.arange(full_rows), full_rows)
    rounded = parent_rows.astype(bf16).astype(np.float32)
    rounded = np.concatenate([rounded, rounded[:tile_rows]], 0)
    child_rows = basis_table(np.arange(3 * full_rows), full_rows)
    row_table = np.zeros((3 * full_rows + tile_rows, 2 * BASIS), np.float32)
    row_table[: 2 * full_rows + tile_rows, :BASIS] = np.concatenate([rounded, parent_rows], 0)
    row_table[:, BASIS:] = np.concatenate([child_rows, child_rows[:tile_rows]], 0)
    child_cols = basis_table((np.arange(3 * full_cols) - 1) % (3 * full_cols), full_cols)
    spread_rows = np.concatenate([child_cols, cols], 0).reshape(-1, tile_cols, BASIS)
    spread_rows = spread_rows.transpose(0, 2, 1)
    spread_table = np.stack(halves(spread_rows), 1)
    amplitude = math.sqrt(full_rows * full_cols) / BASIS

    def mask_of(group_bits, row_bits, col_bits):
        return (group_bits * row_count + row_bits) * col_count + col_bits

    def exchange(value, mask, odd_mask=None):
        masks = (mask, mask if odd_mask is None else odd_mask)
        count = groups * row_count * col_count
        pairs = [(i, i ^ masks[i.bit_count() % 2]) for i in range(count)]
        return lax.ppermute(value, AXES, pairs)

    flip = mask_of(1, 0, 0)
    across = [mask_of(1 << k, 0, 0) ^ flip for k in range(1, groups.bit_length() - 1)]
    across += [mask_of(0, 0, 1 << k) ^ flip for k in range(col_count.bit_length() - 1)]
    row_bits = [1 << k for k in reversed(range(row_count.bit_length() - 1))]
    along = [mask_of(0, bit, 0) ^ flip for bit in row_bits]
    along = along[::-1]
    rounds = across + along
    odd_rounds = across[:1] + along[:1] + across[1:] + along[1:]

    averaged, keep, send, tile, spread, rows, places, rate = pl.pallas_call(
        functools.partial(first_kernel, groups, col_count),
        out_shape=(
            pltpu.VMEM((third_rows, levels * third_cols), bf16),
            pltpu.VMEM((tile_rows, 2 * BASIS), f32),
            pltpu.VMEM((tile_rows, 2 * BASIS), f32),
            pltpu.VMEM(tile_in.shape, bf16),
            pltpu.VMEM((2, BASIS, tile_cols), bf16),
            pltpu.VMEM(row_table.shape, f32),
            pltpu.SMEM((levels,), jnp.int32),
            pltpu.SMEM((levels,), f32),
        ),
        in_specs=[ANY] * 6,
        out_specs=(VMEM,) * 6 + (SMEM, SMEM),
        scratch_shapes=[
            pltpu.VMEM((tile_cols, 2 * BASIS), bf16),
            pltpu.VMEM((third_cols // 128, levels, tile_rows, 128), f32),
            pltpu.VMEM((levels // 2, tile_rows, 2 * BASIS), f32),
            pltpu.SMEM((levels,), jnp.int32),
            pltpu.SemaphoreType.DMA((7,)),
        ],
        name="first",
    )(
        tile_in, jnp.asarray(cols_twice), in_hbm(level_index), in_hbm(nudge_rate),
        jnp.asarray(spread_table), jnp.asarray(row_table),
    )

    partner = exchange(send, flip)
    mine = pl.pallas_call(
        functools.partial(coeffs_kernel, full_rows, groups),
        out_shape=pltpu.VMEM((BASIS, 2 * BASIS), f32),
        in_specs=[SMEM, VMEM, VMEM, VMEM],
        out_specs=VMEM,
        name="coeffs",
    )(offset, in_vmem(keep), in_vmem(partner), in_vmem(rows))
    for masks in zip(rounds, odd_rounds):
        mine = mine + exchange(mine, masks[0], masks[1])
    other = exchange(mine, flip)

    pair = exchange(averaged, flip)
    strips = [jnp.where(parity_of_device() == lax.axis_index("grp") % 2, averaged, pair)]
    for step, bit in enumerate(row_bits):
        held = strips[0] if step == 0 else jnp.concatenate(strips, 0)
        strips = [held, exchange(held, mask_of(0, bit, 0) ^ flip)]
    selected, weights, target = pl.pallas_call(
        functools.partial(select_kernel, full_rows, groups, len(row_bits), amplitude),
        out_shape=(
            pltpu.VMEM((tile_rows, levels * third_cols), bf16),
            pltpu.VMEM((tile_rows, 3 * BASIS), bf16),
            pltpu.VMEM((levels // 2, BASIS, 2 * BASIS), f32),
        ),
        in_specs=[SMEM] + [VMEM] * 4,
        out_specs=(VMEM,) * 3,
        name="select",
    )(offset, *(in_vmem(value) for value in (*strips, rows, driving)))
    block_0 = exchange(selected, mask_of(3, 0, 0))
    block_2 = exchange(selected, mask_of(1, 0, 0))
    block_1 = exchange(block_0, mask_of(1, 0, 0))

    def finish(name, coeffs, values, out_shape, out_spec, scratch):
        values = (coeffs, spread, weights, target, *values)
        return pl.pallas_call(
            functools.partial(final_kernel, full_rows, groups, name == "final_own"),
            out_shape=out_shape,
            in_specs=[SMEM] * 3 + [VMEM] * len(values),
            out_specs=out_spec,
            scratch_shapes=[pltpu.VMEM((2 * tile_rows, 6 * BASIS), bf16), *scratch],
        )(offset, places, rate, *(in_vmem(value) for value in values))

    two_levels = (2, tile_rows, tile_cols)
    earlier = finish(
        "final_own", mine, (tile, selected, block_0, block_1, block_2),
        (pltpu.VMEM(two_levels, bf16), pltpu.VMEM(two_levels, f32)), (VMEM, VMEM),
        [pltpu.VMEM(two_levels, f32)],
    )
    result = finish(
        "final_other", other, earlier, jax.ShapeDtypeStruct(tile_in.shape, bf16), ANY,
        [pltpu.VMEM(two_levels, bf16), pltpu.SemaphoreType.DMA((4,))],
    )
    return result[None]


def solution(mesh):
    placed = (P("grp", None, "row", "col"), P(), P(), P(), P())
    sizes = tuple(mesh.shape[axis] for axis in AXES)
    return jax.shard_map(
        functools.partial(per_device, sizes),
        mesh=mesh,
        in_specs=placed,
        out_specs=P("grp", None, "row", "col"),
        check_vma=False,
    )
```
